256 devices in a mesh: groups: 2 (over y), gz: 64 (over x, z), ea: 2 (over core).
Axes of the slice: x: 4, y: 2, z: 16, core: 2. Of those that a mesh axis runs over, the one named last changes fastest.
The devices are a block of a 4x16x16 slice.
Arguments:
- eigvec: bfloat16 [96, 3, 2, 128, 512], P('ea', None, None, ('groups', 'gz')), parts along dimension 3, may hold values from -3 to 3
- links: float32 [3, 3, 3, 2, 128, 512], P(None, None, None, None, ('groups', 'gz')), parts along dimension 4, may hold values from -1.8 to 1.8
- momentum: int32 [6], P('groups'), parts along dimension 0, may hold values from -2 to 2
- weights: int32 [6], P('groups'), parts along dimension 0, may hold values from 1 to 3
- spins: int32 [6, 2], P('groups'), parts along dimension 0, may hold values from 0 to 3
- peram: float32 [8, 4, 2, 96, 96], P('groups'), parts along dimension 0, may hold values from -0.4375 to 0.4375
Outputs:
- baryon_block: float32 [4, 96, 9216], P('groups', 'ea', 'gz'), parts along dimension 0
The draws below stay inside these ranges and needn't reach their ends.
There are 2 independent parts, one for each index of `groups`. The reference program is written for one: setup_inputs(seed, part) draws one part's arguments, and reference() takes and returns one part's arrays. A program takes and returns all parts, laid end to end along the dimension named above; each array names one. Nothing has to cross between parts.
All inputs are finite; a program needn't handle non-finite values.
Results may differ from the reference program's by a relative error of at most 0.0045.
Values may be sent and summed in bfloat16 or wider, within the bound.
A program may use at most 64 MiB of HBM per device.

```python
import math
import jax
import jax.numpy as jnp
from jax import lax

NVEC = 96
LX = 32
LY = 16
NSPIN = 4
PLANE = 512
NZ = 64
VOLUME = 32768


def set_ends(values, stream_key, smallest, largest):
    place = [jax.random.randint(jax.random.fold_in(stream_key, axis), (), 0, length) for axis, length in enumerate(values.shape)]
    longest = values.shape.index(max(values.shape))
    neighbour = place[:longest] + [(place[longest] + 1) % values.shape[longest]] + place[longest + 1:]
    return values.at[tuple(place)].set(smallest).at[tuple(neighbour)].set(largest)


def levels(rng, dims, cuts, least, largest):
    loudness, own = 1.0, jax.random.fold_in(rng, 6)
    for axis_at, blocks in cuts:
        draws = jnp.exp(jax.random.uniform(jax.random.fold_in(own, axis_at), (blocks,), jnp.float32, least / len(cuts), largest / len(cuts)))
        loudness = loudness * jnp.repeat(draws, dims[axis_at] // blocks).reshape([-1 if axis == axis_at else 1 for axis in range(len(dims))])
    return loudness


def scatter_about(rng, shape, scale, limit, split=(), held_as=jnp.bfloat16):
    array = jax.random.normal(rng, shape, jnp.float32) * scale
    if len(split) > 0:
        array = levels(rng, shape, split, -0.22, 0.18) * array
    return jnp.clip(array, min=-limit, max=limit).astype(held_as)


def setup_inputs(seed: int = 0, part: int = 0) -> dict:
    arg_keys = jax.random.split(jax.random.key(seed), 7)
    part_keys = jax.random.split(jax.random.fold_in(arg_keys[6], part), 7)
    eigvec = scatter_about(part_keys[0], (NVEC, 3, 2, NZ, PLANE), 0.5, 3.0, ((0, 2), (3, 64)))
    links = scatter_about(part_keys[1], (3, 3, 3, 2, NZ, PLANE), 0.3, 1.8, ((4, 64),), jnp.float32)
    momentum = jax.random.randint(part_keys[2], (3,), -2, 3).astype(jnp.int32)
    weights = jax.random.randint(part_keys[3], (3,), 1, 4).astype(jnp.int32)
    spins = set_ends(jax.random.randint(part_keys[4], (3, 2), 0, 4), jax.random.fold_in(part_keys[4], 1), 0, 3).astype(jnp.int32)
    peram = scatter_about(part_keys[5], (NSPIN, NSPIN, 2, NVEC, NVEC), (2 * NVEC) ** -0.5, 0.4375, (), jnp.float32)
    return dict(eigvec=eigvec, links=links, momentum=momentum, weights=weights, spins=spins, peram=peram)


def link_apply(link, lattice_field):
    result_real = 0.0
    result_imaginary = 0.0
    for column_slot in range(3):
        gauge_link_real = link[None, :, column_slot, 0]
        gauge_link_imaginary = link[None, :, column_slot, 1]
        vector_real = lattice_field[:, None, column_slot, 0]
        vector_imaginary = lattice_field[:, None, column_slot, 1]
        result_real = result_real + gauge_link_real * vector_real - gauge_link_imaginary * vector_imaginary
        result_imaginary = result_imaginary + gauge_link_real * vector_imaginary + gauge_link_imaginary * vector_real
    return jnp.stack([result_real, result_imaginary], 2)

def adjoint_apply(link, lattice_field):
    result_real = 0.0
    result_imaginary = 0.0
    for column_slot in range(3):
        gauge_link_real = link[None, column_slot, :, 0]
        gauge_link_imaginary = link[None, column_slot, :, 1]
        vector_real = lattice_field[:, None, column_slot, 0]
        vector_imaginary = lattice_field[:, None, column_slot, 1]
        result_real = result_real + gauge_link_real * vector_real + gauge_link_imaginary * vector_imaginary
        result_imaginary = result_imaginary + gauge_link_real * vector_imaginary - gauge_link_imaginary * vector_real
    return jnp.stack([result_real, result_imaginary], 2)

def cross_parts(left_vec, right_vec):
    reals = []
    imags = []
    for first, second in ((1, 2), (2, 0), (0, 1)):
        ar = left_vec[:, :, first, 0]
        ai = left_vec[:, :, first, 1]
        br = left_vec[:, :, second, 0]
        bi = left_vec[:, :, second, 1]
        cr = right_vec[:, :, first, 0]
        ci = right_vec[:, :, first, 1]
        dr = right_vec[:, :, second, 0]
        di = right_vec[:, :, second, 1]
        reals.append(ar * dr - ai * di - (br * cr - bi * ci))
        imags.append(ar * di + ai * dr - (br * ci + bi * cr))
    return jnp.stack([jnp.stack(reals), jnp.stack(imags)])

def mode_product(lattice_field, block, form):
    high = lax.Precision.HIGHEST
    real_part = jnp.einsum(form, lattice_field[0], block[0], precision=high) - jnp.einsum(form, lattice_field[1], block[1], precision=high)
    imag_part = jnp.einsum(form, lattice_field[0], block[1], precision=high) + jnp.einsum(form, lattice_field[1], block[0], precision=high)
    return jnp.stack([real_part, imag_part])

def reference(eigvec, links, momentum, weights, spins, peram):
    vecf = eigvec.astype(jnp.float32)
    shape_full = vecf.shape[:4] + (LY, LX)
    grid = vecf.reshape(shape_full)
    linkgrid = links.reshape(links.shape[:5] + (LY, LX))
    axes_of = (5, 4, 3)
    disp = jnp.zeros(shape_full, jnp.float32)
    for direction in range(3):
        link = linkgrid[direction]
        ahead = jnp.roll(grid, -1, axes_of[direction])
        back = adjoint_apply(link, grid).astype(jnp.bfloat16)
        behind = jnp.roll(back, 1, axes_of[direction])
        behind = lax.optimization_barrier(behind).astype(jnp.float32)
        factor = weights[direction].astype(jnp.float32)
        disp = disp + factor * (link_apply(link, ahead) - behind)
    disp = disp.reshape(vecf.shape)
    sites = jnp.arange(PLANE, dtype=jnp.int32)
    xcoord = sites % LX
    ycoord = sites // LX
    zcoord = jnp.arange(NZ, dtype=jnp.int32)
    two_pi = 2.0 * math.pi
    inplane = (momentum[0] * xcoord).astype(jnp.float32) / LX + (momentum[1] * ycoord).astype(jnp.float32) / LY
    angle = two_pi * inplane[None, :] + two_pi * (momentum[2] * zcoord).astype(jnp.float32)[:, None] / NZ
    cosine = jnp.cos(angle)
    sine = jnp.sin(angle)
    phased_re = cosine * disp[:, :, 0] + sine * disp[:, :, 1]
    phased_im = cosine * disp[:, :, 1] - sine * disp[:, :, 0]
    phased = jnp.stack([phased_re, phased_im], 2).astype(jnp.bfloat16).astype(jnp.float32)
    high = lax.Precision.HIGHEST

    def plane_step(total, planes):
        vplane, dplane = planes
        wmat = cross_parts(vplane[:, None], vplane[None]).astype(jnp.bfloat16)
        wmat = lax.optimization_barrier(wmat).astype(jnp.float32)
        lre = dplane[:, :, 0]
        lim = dplane[:, :, 1]
        ere = jnp.einsum('aks,kbcs->abc', lre, wmat[0], precision=high) - jnp.einsum('aks,kbcs->abc', lim, wmat[1], precision=high)
        eim = jnp.einsum('aks,kbcs->abc', lre, wmat[1], precision=high) + jnp.einsum('aks,kbcs->abc', lim, wmat[0], precision=high)
        return (total + jnp.stack([ere, eim]), None)
    start = jnp.zeros((2, NVEC, NVEC, NVEC), jnp.float32)
    elemental, unused = lax.scan(plane_step, start, (jnp.moveaxis(vecf, 3, 0), jnp.moveaxis(phased, 3, 0)))
    elemental = elemental * (1.0 / math.sqrt(VOLUME))
    blocks = [peram[spins[q, 0], spins[q, 1]] for q in range(3)]
    result = mode_product(elemental, blocks[2], 'abc,cf->abf')
    result = mode_product(result, blocks[1], 'abc,be->aec')
    result = mode_product(result, blocks[0], 'abc,ad->dbc')
    return result.reshape(2, NVEC, NVEC * NVEC)
```

```python
import functools
import math

import jax
import jax.numpy as jnp
from jax import lax
from jax.experimental import pallas as pl
from jax.experimental.pallas import tpu as pltpu
from jax.sharding import Mesh
from jax.sharding import PartitionSpec as P

LX = 32
LY = 16
NX = 4
NZ = 16
GZ = ("gz_0", "gz_1")
GROUPS_GZ = ("groups", "gz_0", "gz_1")
MESH = pl.DeviceIdType.MESH
F32 = jnp.float32
BF16 = jnp.bfloat16
LEAD = 3


def prep_kernel(half, scale, sizes, spins, moms, p0, p1, p2, zc, mix_ref, left_ref, phase_ref):
    del spins
    ea = lax.axis_index("ea")

    def split(ref, at, value):
        high = value.astype(BF16)
        ref[0, at, :] = high
        ref[1, at, :] = (value - high.astype(F32)).astype(BF16)

    n = p0.shape[-1]
    for slot, p in ((0, p1), (1, p2)):
        re = p[0, 0, 0].T
        im = p[0, 0, 1].T
        split(mix_ref.at[slot], slice(0, n), jnp.concatenate([re, -im], 1))
        split(mix_ref.at[slot], slice(n, 2 * n), jnp.concatenate([im, re], 1))
    re = p0[0, 0, 0].T * scale
    im = p0[0, 0, 1].T * scale
    first = ea == 0
    pad = jnp.zeros((128 - 2 * half, 2 * n), F32)
    for own in range(2):
        low, high = slice(0, half), slice(half, 2 * half)
        one, two = (low, high) if own == 0 else (high, low)
        r = jnp.where(first, re[one], re[two])
        i = jnp.where(first, im[one], im[two])
        real = jnp.concatenate([r, -i], 1)
        imag = jnp.concatenate([i, r], 1)
        split(left_ref.at[0], slice(own * 128, own * 128 + 128), jnp.concatenate([real, imag, pad], 0))
        split(left_ref.at[1], slice(own * 128, own * 128 + 128), jnp.concatenate([-imag, real, pad], 0))
    lx, ly, depth = sizes
    sites = lax.broadcasted_iota(jnp.int32, (8, lx * ly), 1)
    xcoord = sites % lx
    ycoord = sites // lx
    two_pi = 2.0 * math.pi
    inplane = (moms[0] * xcoord).astype(F32) / lx + (moms[1] * ycoord).astype(F32) / ly
    along = jnp.full((8, lx * ly), moms[2] * zc[0], jnp.int32).astype(F32)
    angle = two_pi * inplane + two_pi * along / depth
    phase_ref[0] = jnp.cos(angle)
    phase_ref[1] = jnp.sin(angle)


def times(lr, li, vr, vi):
    return lr * vr - li * vi, lr * vi + li * vr


def times_conj(lr, li, vr, vi):
    return lr * vr + li * vi, lr * vi - li * vr


def main_kernel(
    weights, v_ref, links, phase, mix, left, out_ref,
    vall, upper, lower, back, disp, phown, phall, v1, v2, lmat, wbuf,
    grid_in, mine, grid_out, far_in, mid_out, x_in, zsend, zp_in, zm_in,
    halo_s, halo_r, ea_s, ea_r, dd_s, dd_r, fx_s, fx_r, x_s, x_r, zp_s, zp_r, zm_s, zm_r,
):
    ncomp, half, plane = v_ref.shape
    cols = out_ref.shape[0]
    tiles = cols // 16
    per_row = 2 * half // 16
    x = lax.axis_index("gz_0")
    z = lax.axis_index("gz_1")
    e = lax.axis_index("ea")
    nx = lax.axis_size("gz_0")
    nz = lax.axis_size("gz_1")
    sgn = 1 - 2 * e
    xp = lax.rem(x + sgn + nx, nx)
    xm = lax.rem(x - sgn + nx, nx)
    zp = lax.rem(z + 1, nz)
    zm = lax.rem(z + nz - 1, nz)
    partner = {"ea": 1 - e}
    to_xp = {"gz_0": xp}
    to_xm = {"gz_0": xm}
    to_zp = {"gz_1": zp}
    to_zm = {"gz_1": zm}
    gz = x * nz + z
    gup = lax.rem(gz + 1, nx * nz)
    gdn = lax.rem(gz + nx * nz - 1, nx * nz)
    site_up = {"gz_0": gup // nz, "gz_1": lax.rem(gup, nz)}
    site_dn = {"gz_0": gdn // nz, "gz_1": lax.rem(gdn, nz)}

    def remote(src, dst, s, r, to):
        return pltpu.make_async_remote_copy(
            src_ref=src, dst_ref=dst, send_sem=s, recv_sem=r, device_id=to, device_id_type=MESH
        )

    barrier = pltpu.get_barrier_semaphore()
    for to in (partner, to_xp, to_xm, to_zp, to_zm, site_up, site_dn):
        pl.semaphore_signal(barrier, inc=1, device_id=to, device_id_type=MESH)
    pl.semaphore_wait(barrier, 7)

    send_v = remote(v_ref, upper, halo_s.at[0], halo_r.at[0], site_dn)
    send_v.start()
    send_ea = remote(v_ref, vall.at[e], ea_s.at[0], ea_r.at[0], partner)
    send_ea.start()

    rows = 16

    def field(ref, r0):
        return [ref[c, pl.ds(r0, rows), :].astype(F32) for c in range(ncomp)]

    def link(d, row, col, part):
        return links[pl.ds(((d * 3 + row) * 3 + col) * 2 + part, 1), :]

    def apply(d, f):
        out = []
        for row in range(3):
            re, im = 0.0, 0.0
            for col in range(3):
                a, b = times(link(d, row, col, 0), link(d, row, col, 1), f[2 * col], f[2 * col + 1])
                re, im = re + a, im + b
            out += [re, im]
        return out

    def adjoint(d, f):
        out = []
        for col in range(3):
            re, im = 0.0, 0.0
            for row in range(3):
                a, b = times_conj(
                    link(d, row, col, 0), link(d, row, col, 1), f[2 * row], f[2 * row + 1]
                )
                re, im = re + a, im + b
            out += [re, im]
        return out

    def back_tile(t, _):
        r0 = pl.multiple_of(t * rows, rows)
        f = field(v_ref, r0)
        for c, val in enumerate(adjoint(2, f)):
            back[c, pl.ds(r0, rows), :] = val.astype(BF16)
        for c in range(ncomp):
            vall[e, c, pl.ds(r0, rows), :] = v_ref[c, pl.ds(r0, rows), :]
        return 0

    lax.fori_loop(0, half // rows, back_tile, 0)
    send_b = remote(back, lower, halo_s.at[1], halo_r.at[1], site_up)
    send_b.start()

    lane = lax.broadcasted_iota(jnp.int32, (rows, plane), 1)
    xc = lax.rem(lane, LX)

    def shift_x(val, by):
        if by < 0:
            return jnp.where(
                xc == LX - 1, pltpu.roll(val, LX - 1, 1), pltpu.roll(val, plane - 1, 1)
            )
        return jnp.where(xc == 0, pltpu.roll(val, plane - (LX - 1), 1), pltpu.roll(val, 1, 1))

    def shift_y(val, by):
        return pltpu.roll(val, plane - LX if by < 0 else LX, 1)

    def inplane_tile(t, _):
        r0 = pl.multiple_of(t * rows, rows)
        for d, shift in ((0, shift_x), (1, shift_y)):
            f = field(v_ref, r0)
            ahead = apply(d, [shift(c, -1) for c in f])
            behind = [shift(c.astype(BF16).astype(F32), 1) for c in adjoint(d, f)]
            for c in range(ncomp):
                term = weights[d].astype(F32) * (ahead[c] - behind[c])
                if d == 0:
                    disp[c, pl.ds(r0, rows), :] = term
                else:
                    disp[c, pl.ds(r0, rows), :] += term
        return 0

    lax.fori_loop(0, half // rows, inplane_tile, 0)

    send_ea.wait()
    for slot, dst in ((0, v1), (1, v2)):
        for k in range(3):
            stack = jnp.concatenate(
                [vall[0, 2 * k], vall[1, 2 * k], vall[0, 2 * k + 1], vall[1, 2 * k + 1]], 0
            )
            res = jnp.dot(mix[slot, 0], stack, preferred_element_type=F32) + jnp.dot(
                mix[slot, 1], stack, preferred_element_type=F32
            )
            for r in range(2):
                part = res[2 * half * r : 2 * half * (r + 1)]
                for lt in range(plane // 128):
                    dst[2 * k + r, lt] = part[:, lt * 128 : lt * 128 + 128]

    send_v.wait()
    send_b.wait()
    cosine = phase[0, 0:1]
    sine = phase[1, 0:1]

    def zdir_tile(t, _):
        r0 = pl.multiple_of(t * rows, rows)
        ahead = apply(2, field(upper, r0))
        low = field(lower, r0)
        tot = [
            disp[c, pl.ds(r0, rows), :] + weights[2].astype(F32) * (ahead[c] - low[c])
            for c in range(ncomp)
        ]
        for k in range(3):
            re, im = tot[2 * k], tot[2 * k + 1]
            phown[2 * k, pl.ds(r0, rows), :] = (cosine * re + sine * im).astype(BF16)
            phown[2 * k + 1, pl.ds(r0, rows), :] = (cosine * im - sine * re).astype(BF16)
        for c in range(ncomp):
            phall[e, c, pl.ds(r0, rows), :] = phown[c, pl.ds(r0, rows), :]
        return 0

    lax.fori_loop(0, half // rows, zdir_tile, 0)
    send_ph = remote(phown, phall.at[e], ea_s.at[1], ea_r.at[1], partner)
    send_ph.start()
    send_ph.wait()
    for k in range(3):
        stack = jnp.concatenate(
            [phall[0, 2 * k], phall[1, 2 * k], phall[0, 2 * k + 1], phall[1, 2 * k + 1]], 0
        )
        for r in range(2):
            res = jnp.dot(left[r, 0], stack, preferred_element_type=F32) + jnp.dot(
                left[r, 1], stack, preferred_element_type=F32
            )
            lmat[pl.ds((2 * k + r) * plane, plane), :] = res.T.astype(BF16)

    def dest_z(q):
        step = q // 2
        return lax.rem(jnp.where(lax.rem(q, 2) == 0, z + 8 - step, z - 7 + step) + nz, nz)

    def w_tile(t, zd, blk):
        xd = lax.rem(jnp.where(blk == 0, x + sgn + nx, x + 2 * (1 - e)), nx)
        at = (xd * nz + zd) * tiles + t
        b2 = at // per_row
        c0 = pl.multiple_of(lax.rem(at, per_row) * 16, 16)
        row0 = pl.multiple_of(t * 16, 16)
        for lt in range(plane // 128):
            b = [v1[c, lt, pl.ds(b2, 16, stride=0), :] for c in range(ncomp)]
            w = [v2[c, lt, pl.ds(c0, 16), :] for c in range(ncomp)]
            for k, (i, j) in enumerate(((1, 2), (2, 0), (0, 1))):
                ar, ai, br, bi = b[2 * i], b[2 * i + 1], b[2 * j], b[2 * j + 1]
                cr, ci, dr, di = w[2 * i], w[2 * i + 1], w[2 * j], w[2 * j + 1]
                re = ar * dr - ai * di - (br * cr - bi * ci)
                im = ar * di + ai * dr - (br * ci + bi * cr)
                at_re = (2 * k) * plane + lt * 128
                at_im = (2 * k + 1) * plane + lt * 128
                wbuf[pl.ds(row0, 16), at_re : at_re + 128] = re.astype(BF16)
                wbuf[pl.ds(row0, 16), at_im : at_im + 128] = im.astype(BF16)

    def to_partner(q, blk):
        role = 1 if blk == 0 else 2 + e
        return remote(
            grid_out.at[q, blk], grid_in.at[q, role], dd_s.at[q, blk], dd_r.at[q, blk], partner
        )

    def compute(q):
        zd = dest_z(q)
        for blk in range(2):
            lax.fori_loop(0, tiles, lambda t, c: (w_tile(t, zd, blk), 0)[1], 0)
            res = jnp.dot(wbuf[...], lmat[...], preferred_element_type=F32)
            grid_out[q, blk] = res[:, 128:].astype(BF16)
            to_partner(q, blk).start()
            mine[q, blk] = res[:, :128].astype(BF16)

    def far_copy(q):
        return remote(grid_in.at[q, 2], far_in.at[q], fx_s.at[q], fx_r.at[q], to_xp)

    def far_mine(q):
        return remote(mine.at[q, 1], far_in.at[q], fx_s.at[q], fx_r.at[q], to_xp)

    def direct_copy(q):
        return remote(grid_in.at[q, 1], x_in.at[q, 0], x_s.at[q, 0], x_r.at[q, 0], to_xm)

    def mid_copy(q):
        return remote(mid_out.at[q], x_in.at[q, 1], x_s.at[q, 1], x_r.at[q, 1], to_xp)

    def first_x(q):
        to_partner(q, 0).wait_recv()
        to_partner(q, 1).wait_recv()

        @pl.when(e == 0)
        def _():
            far_mine(q).start()

        @pl.when(e == 1)
        def _():
            far_copy(q).start()

        direct_copy(q).start()

    def second_x(q):
        far_mine(q).wait_recv()
        mid_out[q] = (mine[q, 0].astype(F32) + far_in[q].astype(F32)).astype(BF16)
        mid_copy(q).start()

    def x_sum(q):
        direct_copy(q).wait_recv()
        mid_copy(q).wait_recv()
        total = x_in[q, 0].astype(F32) + x_in[q, 1].astype(F32)
        own = jnp.where(e == 0, grid_in[q, 3].astype(F32), mine[q, 1].astype(F32))
        return total + own

    def plus_copy(step):
        return remote(zsend.at[0, step], zp_in.at[step], zp_s.at[step], zp_r.at[step], to_zp)

    def minus_copy(step):
        return remote(zsend.at[1, step], zm_in.at[step], zm_s.at[step], zm_r.at[step], to_zm)

    last = 7

    def ring(step):
        zsend[0, step] = x_sum(2 * step)
        zsend[1, step] = x_sum(2 * step + 1)

        @pl.when(step > 0)
        def _():
            plus_copy(step - 1).wait_recv()
            zsend[0, step] += zp_in[step - 1]

        plus_copy(step).start()

        @pl.when(step > 0)
        def _():
            minus_copy(step - 1).wait_recv()
            zsend[1, step] += zm_in[step - 1]

        @pl.when(step < last)
        def _():
            minus_copy(step).start()

    def body(i, _):
        @pl.when(i <= last)
        def _():
            compute(2 * i)
            compute(2 * i + 1)

        @pl.when((i >= 1) & (i <= last + 1))
        def _():
            first_x(2 * (i - 1))
            first_x(2 * (i - 1) + 1)

        @pl.when((i >= 2) & (i <= last + 2))
        def _():
            second_x(2 * (i - 2))
            second_x(2 * (i - 2) + 1)

        @pl.when(i >= 3)
        def _():
            ring(i - 3)

        return 0

    lax.fori_loop(0, last + 4, body, 0)
    plus_copy(last).wait_recv()
    out_ref[...] = zsend[1, last] + zp_in[last]

    def drain(q, _):
        to_partner(q, 0).wait_send()
        to_partner(q, 1).wait_send()
        far_mine(q).wait_send()
        direct_copy(q).wait_send()
        mid_copy(q).wait_send()
        return 0

    lax.fori_loop(0, 2 * (last + 1), drain, 0)
    for step in range(last + 1):
        plus_copy(step).wait_send()
        if step < last:
            minus_copy(step).wait_send()


def shards(eigvec, links, momentum, weights, spins, peram):
    half = eigvec.shape[0]
    plane = eigvec.shape[4]
    n = 2 * half
    nx, nz, cores = lax.axis_size("gz_0"), lax.axis_size("gz_1"), lax.axis_size("ea")
    depth = nx * nz
    cols = n * n // depth
    scale = 1.0 / math.sqrt(LX * LY * depth)
    zcoord = lax.axis_index(GZ).astype(jnp.int32).reshape(1)

    def block_of(q):
        return pl.BlockSpec((1, 1, 2, n, n), lambda i, sp, mo: (sp[q, 0], sp[q, 1], 0, 0, 0))

    mix, left, phase = pl.pallas_call(
        functools.partial(prep_kernel, half, scale, (LX, LY, depth)),
        grid_spec=pltpu.PrefetchScalarGridSpec(
            num_scalar_prefetch=2,
            grid=(1,),
            in_specs=[block_of(0), block_of(1), block_of(2), pl.BlockSpec(memory_space=pltpu.SMEM)],
            out_specs=[
                pl.BlockSpec((2, 2, 2 * n, 2 * n), lambda i, sp, mo: (0, 0, 0, 0)),
                pl.BlockSpec((2, 2, 256, 2 * n), lambda i, sp, mo: (0, 0, 0, 0)),
                pl.BlockSpec((2, 8, plane), lambda i, sp, mo: (0, 0, 0)),
            ],
        ),
        out_shape=[
            jax.ShapeDtypeStruct((2, 2, 2 * n, 2 * n), BF16),
            jax.ShapeDtypeStruct((2, 2, 256, 2 * n), BF16),
            jax.ShapeDtypeStruct((2, 8, plane), F32),
        ],
    )(spins, momentum, peram, peram, peram, zcoord)

    fields = eigvec.reshape(half, 6, plane).transpose(1, 0, 2)
    link_rows = links.reshape(54, plane)
    vm = pl.BlockSpec(memory_space=pltpu.VMEM)
    dma = pltpu.SemaphoreType.DMA
    nq = nz
    out = pl.pallas_call(
        main_kernel,
        out_shape=jax.ShapeDtypeStruct((cols, 128), F32),
        in_specs=[pl.BlockSpec(memory_space=pltpu.SMEM)] + [vm] * 5,
        out_specs=vm,
        scratch_shapes=[
            pltpu.VMEM((2, 6, half, plane), BF16),
            pltpu.VMEM((6, half, plane), BF16),
            pltpu.VMEM((6, half, plane), BF16),
            pltpu.VMEM((6, half, plane), BF16),
            pltpu.VMEM((6, half, plane), F32),
            pltpu.VMEM((6, half, plane), BF16),
            pltpu.VMEM((2, 6, half, plane), BF16),
            pltpu.VMEM((6, plane // 128, n, 128), F32),
            pltpu.VMEM((6, plane // 128, n, 128), F32),
            pltpu.VMEM((6 * plane, 256), BF16),
            pltpu.VMEM((cols, 6 * plane), BF16),
            pltpu.VMEM((nq, 4, cols, 128), BF16),
            pltpu.VMEM((nq, 2, cols, 128), BF16),
            pltpu.VMEM((nq, 2, cols, 128), BF16),
            pltpu.VMEM((nq, cols, 128), BF16),
            pltpu.VMEM((nq, cols, 128), BF16),
            pltpu.VMEM((nq, 2, cols, 128), BF16),
            pltpu.VMEM((2, 8, cols, 128), F32),
            pltpu.VMEM((8, cols, 128), F32),
            pltpu.VMEM((8, cols, 128), F32),
            dma((2,)), dma((2,)), dma((2,)), dma((2,)),
            dma((nq, 2)), dma((nq, 2)), dma((nq,)), dma((nq,)),
            dma((nq, 2)), dma((nq, 2)), dma((8,)), dma((8,)), dma((8,)), dma((8,)),
        ],
        compiler_params=pltpu.CompilerParams(
            collective_id=0, has_side_effects=True, vmem_limit_bytes=60 * 1024 * 1024
        ),
    )(weights, fields, link_rows, phase, mix, left)
    return out[:, :n].reshape(cols, 2, half).transpose(1, 2, 0)


def solution(mesh):
    split = Mesh(
        mesh.devices.reshape(mesh.shape["groups"], NX, NZ, mesh.shape["ea"]),
        ("groups", "gz_0", "gz_1", "ea"),
    )
    in_specs = (
        P("ea", None, None, GROUPS_GZ, None),
        P(None, None, None, None, GROUPS_GZ, None),
        P("groups"),
        P("groups"),
        P("groups", None),
        P("groups", None, None, None, None),
    )
    out_specs = P("groups", "ea", GZ)
    return jax.shard_map(
        shards, mesh=split, in_specs=in_specs, out_specs=out_specs, check_vma=False
    )
```

```python
import functools
import math

import jax
import jax.numpy as jnp
from jax import lax
from jax.experimental import pallas as pl
from jax.experimental.pallas import tpu as pltpu
from jax.sharding import Mesh
from jax.sharding import PartitionSpec as P

LX = 32
LY = 16
NX = 4
NZ = 16
SIDE = 4
GZ = ("gz_0", "gz_1")
GROUPS_GZ = ("groups", "gz_0", "gz_1")
MESH = pl.DeviceIdType.MESH
F32 = jnp.float32
BF16 = jnp.bfloat16


def prep_kernel(half, scale, sizes, spins, moms, p0, p1, p2, zc, mix_ref, left_ref, phase_ref):
    del spins
    ea = lax.axis_index("ea")

    def split(ref, at, value):
        high = value.astype(BF16)
        ref[0, at, :] = high
        ref[1, at, :] = (value - high.astype(F32)).astype(BF16)

    n = p0.shape[-1]
    for slot, p in ((0, p1), (1, p2)):
        re = p[0, 0, 0].T
        im = p[0, 0, 1].T
        split(mix_ref.at[slot], slice(0, n), jnp.concatenate([re, -im], 1))
        split(mix_ref.at[slot], slice(n, 2 * n), jnp.concatenate([im, re], 1))
    re = p0[0, 0, 0].T * scale
    im = p0[0, 0, 1].T * scale
    first = ea == 0
    pad = jnp.zeros((128 - 2 * half, 2 * n), F32)
    for own in range(2):
        low, high = slice(0, half), slice(half, 2 * half)
        one, two = (low, high) if own == 0 else (high, low)
        r = jnp.where(first, re[one], re[two])
        i = jnp.where(first, im[one], im[two])
        real = jnp.concatenate([r, -i], 1)
        imag = jnp.concatenate([i, r], 1)
        split(left_ref.at[0], slice(own * 128, own * 128 + 128), jnp.concatenate([real, imag, pad], 0))
        split(left_ref.at[1], slice(own * 128, own * 128 + 128), jnp.concatenate([-imag, real, pad], 0))
    lx, ly, depth = sizes
    sites = lax.broadcasted_iota(jnp.int32, (8, lx * ly), 1)
    xcoord = sites % lx
    ycoord = sites // lx
    two_pi = 2.0 * math.pi
    inplane = (moms[0] * xcoord).astype(F32) / lx + (moms[1] * ycoord).astype(F32) / ly
    along = jnp.full((8, lx * ly), moms[2] * zc[0], jnp.int32).astype(F32)
    angle = two_pi * inplane + two_pi * along / depth
    phase_ref[0] = jnp.cos(angle)
    phase_ref[1] = jnp.sin(angle)


def times(lr, li, vr, vi):
    return lr * vr - li * vi, lr * vi + li * vr


def times_conj(lr, li, vr, vi):
    return lr * vr + li * vi, lr * vi - li * vr


def main_kernel(
    weights, v_ref, links, phase, mix, left, out_ref,
    vall, upper, lower, back, disp, phown, phall, v1, v2, lmat, wbuf0, wbuf1, acc,
    grid_in, mine, grid_out, far_in, mid_out, x_in, near_out, near_in, near_own, long_out, long_in,
    halo_s, halo_r, ea_s, ea_r, dd_s, dd_r, fx_s, fx_r, x_s, x_r, near_s, near_r, long_s, long_r,
):
    ncomp, half, plane = v_ref.shape
    cols = out_ref.shape[0]
    packed = far_in.shape[1]
    tiles = cols // 16
    per_row = 2 * half // 16
    x = lax.axis_index("gz_0")
    z = lax.axis_index("gz_1")
    e = lax.axis_index("ea")
    nx = lax.axis_size("gz_0")
    nz = lax.axis_size("gz_1")
    sgn = 1 - 2 * e
    xp = lax.rem(x + sgn + nx, nx)
    xm = lax.rem(x - sgn + nx, nx)
    zh = z // SIDE
    zl = lax.rem(z, SIDE)
    partner = {"ea": 1 - e}
    to_xp = {"gz_0": xp}
    to_xm = {"gz_0": xm}
    gz = x * nz + z
    gup = lax.rem(gz + 1, nx * nz)
    gdn = lax.rem(gz + nx * nz - 1, nx * nz)
    site_up = {"gz_0": gup // nz, "gz_1": lax.rem(gup, nz)}
    site_dn = {"gz_0": gdn // nz, "gz_1": lax.rem(gdn, nz)}

    def in_side(r):
        return {"gz_1": zh * SIDE + lax.rem(zl + r, SIDE)}

    def across(r):
        return {"gz_1": lax.rem(zh + r, SIDE) * SIDE + zl}

    def turn_of(n):
        return jnp.where(n == 0, 2, jnp.where(n == 1, 1, jnp.where(n == 2, 3, 0)))

    def remote(src, dst, s, r, to):
        return pltpu.make_async_remote_copy(
            src_ref=src, dst_ref=dst, send_sem=s, recv_sem=r, device_id=to, device_id_type=MESH
        )

    barrier = pltpu.get_barrier_semaphore()
    peers = [partner, to_xp, to_xm, site_up, site_dn]
    for r in range(1, SIDE):
        peers.append(in_side(r))
        peers.append(across(r))
    for to in peers:
        pl.semaphore_signal(barrier, inc=1, device_id=to, device_id_type=MESH)
    pl.semaphore_wait(barrier, len(peers))

    send_v = remote(v_ref, upper, halo_s.at[0], halo_r.at[0], site_dn)
    send_v.start()
    send_ea = remote(v_ref, vall.at[e], ea_s.at[0], ea_r.at[0], partner)
    send_ea.start()

    rows = 16

    def field(ref, r0):
        return [ref[c, pl.ds(r0, rows), :].astype(F32) for c in range(ncomp)]

    def link(d, row, col, part):
        return links[((d * 3 + row) * 3 + col) * 2 + part]

    def apply(d, f):
        out = []
        for row in range(3):
            re, im = 0.0, 0.0
            for col in range(3):
                a, b = times(link(d, row, col, 0), link(d, row, col, 1), f[2 * col], f[2 * col + 1])
                re, im = re + a, im + b
            out += [re, im]
        return out

    def adjoint(d, f):
        out = []
        for col in range(3):
            re, im = 0.0, 0.0
            for row in range(3):
                a, b = times_conj(
                    link(d, row, col, 0), link(d, row, col, 1), f[2 * row], f[2 * row + 1]
                )
                re, im = re + a, im + b
            out += [re, im]
        return out

    def back_tile(t, _):
        r0 = pl.multiple_of(t * rows, rows)
        f = field(v_ref, r0)
        for c, val in enumerate(adjoint(2, f)):
            back[c, pl.ds(r0, rows), :] = val.astype(BF16)
        for c in range(ncomp):
            vall[e, c, pl.ds(r0, rows), :] = v_ref[c, pl.ds(r0, rows), :]
        return 0

    lax.fori_loop(0, half // rows, back_tile, 0)
    send_b = remote(back, lower, halo_s.at[1], halo_r.at[1], site_up)
    send_b.start()

    lane = lax.broadcasted_iota(jnp.int32, (rows, plane), 1)
    xc = lax.rem(lane, LX)

    def shift_x(val, by):
        if by < 0:
            return jnp.where(
                xc == LX - 1, pltpu.roll(val, LX - 1, 1), pltpu.roll(val, plane - 1, 1)
            )
        return jnp.where(xc == 0, pltpu.roll(val, plane - (LX - 1), 1), pltpu.roll(val, 1, 1))

    def shift_y(val, by):
        return pltpu.roll(val, plane - LX if by < 0 else LX, 1)

    def inplane_tile(t, _):
        r0 = pl.multiple_of(t * rows, rows)
        for d, shift in ((0, shift_x), (1, shift_y)):
            f = field(v_ref, r0)
            ahead = apply(d, [shift(c, -1) for c in f])
            behind = [shift(c.astype(BF16).astype(F32), 1) for c in adjoint(d, f)]
            for c in range(ncomp):
                term = weights[d].astype(F32) * (ahead[c] - behind[c])
                if d == 0:
                    disp[c, pl.ds(r0, rows), :] = term
                else:
                    disp[c, pl.ds(r0, rows), :] += term
        return 0

    send_ea.wait()
    for slot, dst in ((0, v1), (1, v2)):
        for k in range(3):
            stack = jnp.concatenate(
                [vall[0, 2 * k], vall[1, 2 * k], vall[0, 2 * k + 1], vall[1, 2 * k + 1]], 0
            )
            res = jnp.dot(mix[slot, 0], stack, preferred_element_type=F32) + jnp.dot(
                mix[slot, 1], stack, preferred_element_type=F32
            )
            for r in range(2):
                part = res[2 * half * r : 2 * half * (r + 1)]
                for lt in range(plane // 128):
                    dst[2 * k + r, lt] = part[:, lt * 128 : lt * 128 + 128]

    def dest_z(q):
        hop = lax.rem(zh + turn_of(q // SIDE), SIDE)
        return hop * SIDE + lax.rem(zl + turn_of(lax.rem(q, SIDE)), SIDE)

    turns = 4

    def w_section(dst, step, sec):
        par = sec // 2
        blk = sec - 2 * par
        xd = lax.rem(jnp.where(blk == 0, x + sgn + nx, x + 2 * (1 - e)), nx)
        first = (xd * nz + dest_z(2 * step + par)) * tiles
        row = first // per_row
        skip = first - row * per_row
        for t in range(tiles):
            u = skip + t
            over = jnp.where(u >= per_row, 1, 0) + jnp.where(u >= 2 * per_row, 1, 0)
            b2 = row + over
            c0 = pl.multiple_of((u - over * per_row) * 16, 16)
            row0 = pl.multiple_of(sec * cols + t * 16, 16)
            for lt in range(plane // 128):
                b = [v1[c, lt, pl.ds(b2, 16, stride=0), :] for c in range(ncomp)]
                w = [v2[c, lt, pl.ds(c0, 16), :] for c in range(ncomp)]
                for k, (i, j) in enumerate(((1, 2), (2, 0), (0, 1))):
                    ar, ai, br, bi = b[2 * i], b[2 * i + 1], b[2 * j], b[2 * j + 1]
                    cr, ci, dr, di = w[2 * i], w[2 * i + 1], w[2 * j], w[2 * j + 1]
                    re = ar * dr - ai * di - (br * cr - bi * ci)
                    im = ar * di + ai * dr - (br * ci + bi * cr)
                    for r, val in ((0, re), (1, im)):
                        piece = 2 * (2 * k + r) + lt // 2
                        at = (piece % 3) * 256 + (lt % 2) * 128
                        dst[piece // 3, pl.ds(row0, 16), at : at + 128] = val.astype(BF16)

    def w_only(dst, step):
        lax.fori_loop(0, turns, lambda k, c: (w_section(dst, step, k), 0)[1], 0)

    def dot_turn(src, k):
        acc[...] += jnp.dot(src[k], lmat[k], preferred_element_type=F32)

    def fused(src, dst, step):
        acc[...] = jnp.zeros_like(acc)

        def turn(k, _):
            dot_turn(src, k)
            w_section(dst, step + 1, k)
            return 0

        lax.fori_loop(0, turns, turn, 0)

    def dot_only(src):
        acc[...] = jnp.zeros_like(acc)
        lax.fori_loop(0, turns, lambda k, c: (dot_turn(src, k), 0)[1], 0)

    def to_partner(q, blk):
        role = 1 if blk == 0 else 2 + e
        return remote(
            grid_out.at[q, blk], grid_in.at[q, role], dd_s.at[q, blk], dd_r.at[q, blk], partner
        )

    fill = lax.broadcasted_iota(jnp.int32, (32, 128), 1) < 2 * half

    def pack(rows_at, lanes):
        for g in range(3):
            extra = acc[rows_at + packed : rows_at + cols, lanes]
            extra = pltpu.roll(extra, 2 * half - 32 * g, 1)
            yield jnp.where(fill, acc[rows_at + 32 * g : rows_at + 32 * g + 32, lanes], extra)
        yield acc[rows_at + 96 : rows_at + packed, lanes]

    def put(ref, pieces):
        at = 0
        for piece in pieces:
            ref[at : at + piece.shape[0], :] = piece.astype(BF16)
            at += piece.shape[0]

    def give(step):
        for par in range(2):
            for blk in range(2):
                q = 2 * step + par
                rows_at = (2 * par + blk) * cols
                put(grid_out.at[q, blk], pack(rows_at, slice(128, 256)))
                to_partner(q, blk).start()
                put(mine.at[q, blk], pack(rows_at, slice(0, 128)))

    def far_copy(q):
        return remote(grid_in.at[q, 2], far_in.at[q], fx_s.at[q], fx_r.at[q], to_xp)

    def far_mine(q):
        return remote(mine.at[q, 1], far_in.at[q], fx_s.at[q], fx_r.at[q], to_xp)

    def direct_copy(q):
        return remote(grid_in.at[q, 1], x_in.at[q, 0], x_s.at[q, 0], x_r.at[q, 0], to_xm)

    def mid_copy(q):
        return remote(mid_out.at[q], x_in.at[q, 1], x_s.at[q, 1], x_r.at[q, 1], to_xp)

    def first_x(q):
        to_partner(q, 0).wait_recv()
        to_partner(q, 1).wait_recv()

        @pl.when(e == 0)
        def _():
            far_mine(q).start()

        @pl.when(e == 1)
        def _():
            far_copy(q).start()

        direct_copy(q).start()

    def second_x(q):
        far_mine(q).wait_recv()
        mid_out[q] = (mine[q, 0].astype(F32) + far_in[q].astype(F32)).astype(BF16)
        mid_copy(q).start()

    def x_sum(q):
        direct_copy(q).wait_recv()
        mid_copy(q).wait_recv()
        total = x_in[q, 0].astype(F32) + x_in[q, 1].astype(F32)
        own = jnp.where(e == 0, grid_in[q, 3].astype(F32), mine[q, 1].astype(F32))
        return total + own

    last = 7

    def near_copy(q, g, r):
        return remote(near_out.at[q], near_in.at[g, r], near_s.at[q], near_r.at[g, r], in_side(r))

    def near_sum(step):
        for par in range(2):
            q = 2 * step + par
            g = q // SIDE
            r = turn_of(lax.rem(q, SIDE))
            total = x_sum(q)
            if par == 0:
                near_out[q] = total.astype(BF16)
                near_copy(q, g, r).start()
            else:

                @pl.when(r > 0)
                def _():
                    near_out[q] = total.astype(BF16)
                    near_copy(q, g, r).start()

                @pl.when(r == 0)
                def _():
                    near_own[g] = total

    def long_copy(g):
        return remote(
            long_out.at[g], long_in.at[g], long_s.at[g], long_r.at[g], across(turn_of(g))
        )

    def long_sum(g):
        total = near_own[g]
        for r in range(1, SIDE):
            near_copy(0, g, r).wait_recv()
            total = total + near_in[g, r].astype(F32)
        near_own[g] = total

        @pl.when(g < SIDE - 1)
        def _():
            long_out[g] = near_own[g]
            long_copy(g).start()

    w_only(wbuf0, 0)
    lax.fori_loop(0, half // rows, inplane_tile, 0)
    send_v.wait()
    send_b.wait()
    cosine = phase[0, 0:1]
    sine = phase[1, 0:1]

    def zdir_tile(t, _):
        r0 = pl.multiple_of(t * rows, rows)
        ahead = apply(2, field(upper, r0))
        low = field(lower, r0)
        tot = [
            disp[c, pl.ds(r0, rows), :] + weights[2].astype(F32) * (ahead[c] - low[c])
            for c in range(ncomp)
        ]
        for k in range(3):
            re, im = tot[2 * k], tot[2 * k + 1]
            phown[2 * k, pl.ds(r0, rows), :] = (cosine * re + sine * im).astype(BF16)
            phown[2 * k + 1, pl.ds(r0, rows), :] = (cosine * im - sine * re).astype(BF16)
        for c in range(ncomp):
            phall[e, c, pl.ds(r0, rows), :] = phown[c, pl.ds(r0, rows), :]
        return 0

    lax.fori_loop(0, half // rows, zdir_tile, 0)
    send_ph = remote(phown, phall.at[e], ea_s.at[1], ea_r.at[1], partner)
    send_ph.start()
    send_ph.wait()
    for k in range(3):
        stack = jnp.concatenate(
            [phall[0, 2 * k], phall[1, 2 * k], phall[0, 2 * k + 1], phall[1, 2 * k + 1]], 0
        )
        for r in range(2):
            res = jnp.dot(left[r, 0], stack, preferred_element_type=F32) + jnp.dot(
                left[r, 1], stack, preferred_element_type=F32
            )
            turned = res.T.astype(BF16)
            for hf in range(2):
                piece = 2 * (2 * k + r) + hf
                at = (piece % 3) * 256
                lmat[piece // 3, at : at + 256, :] = turned[hf * 256 : hf * 256 + 256]

    def stage(step, src, dst):
        @pl.when(step < last)
        def _():
            fused(src, dst, step)

        @pl.when(step == last)
        def _():
            dot_only(src)

        @pl.when((step >= 1) & (step <= last + 1))
        def _():
            first_x(2 * (step - 1))
            first_x(2 * (step - 1) + 1)

        @pl.when(step <= last)
        def _():
            give(step)

        @pl.when((step >= 3) & (step <= last + 3))
        def _():
            second_x(2 * (step - 3))
            second_x(2 * (step - 3) + 1)

        @pl.when((step >= 5) & (step <= last + 5))
        def _():
            near_sum(step - 5)

    def body(i, _):
        stage(2 * i, wbuf0, wbuf1)

        stage(2 * i + 1, wbuf1, wbuf0)

        @pl.when(i >= 3)
        def _():
            long_sum(i - 3)

        return 0

    lax.fori_loop(0, 7, body, 0)
    total = near_own[SIDE - 1]
    for g in range(SIDE - 1):
        long_copy(g).wait_recv()
        total = total + long_in[g]
    out_ref[0:packed, :] = total
    spot = lax.broadcasted_iota(jnp.int32, (32, 128), 1)
    extra = jnp.zeros((32, 128), F32)
    for g in range(3):
        piece = pltpu.roll(total[32 * g : 32 * g + 32], (128 - 2 * half + 32 * g) % 128, 1)
        extra = jnp.where((spot >= 32 * g) & (spot < 32 * g + 32), piece, extra)
    out_ref[packed:cols, :] = extra

    def drain(q, _):
        to_partner(q, 0).wait_send()
        to_partner(q, 1).wait_send()
        far_mine(q).wait_send()
        direct_copy(q).wait_send()
        mid_copy(q).wait_send()

        @pl.when(lax.rem(q, SIDE) < SIDE - 1)
        def _():
            near_copy(q, 0, 1).wait_send()

        return 0

    lax.fori_loop(0, 2 * (last + 1), drain, 0)
    for g in range(SIDE - 1):
        long_copy(g).wait_send()


def shards(eigvec, links, momentum, weights, spins, peram):
    half = eigvec.shape[0]
    plane = eigvec.shape[4]
    n = 2 * half
    nx, nz, cores = lax.axis_size("gz_0"), lax.axis_size("gz_1"), lax.axis_size("ea")
    depth = nx * nz
    cols = n * n // depth
    scale = 1.0 / math.sqrt(LX * LY * depth)
    zcoord = lax.axis_index(GZ).astype(jnp.int32).reshape(1)

    def block_of(q):
        return pl.BlockSpec((1, 1, 2, n, n), lambda i, sp, mo: (sp[0, q], sp[1, q], 0, 0, 0))

    mix, left, phase = pl.pallas_call(
        functools.partial(prep_kernel, half, scale, (LX, LY, depth)),
        grid_spec=pltpu.PrefetchScalarGridSpec(
            num_scalar_prefetch=2,
            grid=(1,),
            in_specs=[block_of(0), block_of(1), block_of(2), pl.BlockSpec(memory_space=pltpu.SMEM)],
            out_specs=[
                pl.BlockSpec((2, 2, 2 * n, 2 * n), lambda i, sp, mo: (0, 0, 0, 0)),
                pl.BlockSpec((2, 2, 256, 2 * n), lambda i, sp, mo: (0, 0, 0, 0)),
                pl.BlockSpec((2, 8, plane), lambda i, sp, mo: (0, 0, 0)),
            ],
        ),
        out_shape=[
            jax.ShapeDtypeStruct((2, 2, 2 * n, 2 * n), BF16),
            jax.ShapeDtypeStruct((2, 2, 256, 2 * n), BF16),
            jax.ShapeDtypeStruct((2, 8, plane), F32),
        ],
    )(spins.T, momentum, peram, peram, peram, zcoord)

    fields = eigvec.reshape(half, 6, plane).transpose(1, 0, 2)
    link_rows = links.reshape(54, 1, plane)
    vm = pl.BlockSpec(memory_space=pltpu.VMEM)
    dma = pltpu.SemaphoreType.DMA
    nq = nz
    packed = cols - 32
    out = pl.pallas_call(
        main_kernel,
        out_shape=jax.ShapeDtypeStruct((cols, 128), F32),
        in_specs=[pl.BlockSpec(memory_space=pltpu.SMEM)] + [vm] * 5,
        out_specs=vm,
        scratch_shapes=[
            pltpu.VMEM((2, 6, half, plane), BF16),
            pltpu.VMEM((6, half, plane), BF16),
            pltpu.VMEM((6, half, plane), BF16),
            pltpu.VMEM((6, half, plane), BF16),
            pltpu.VMEM((6, half, plane), F32),
            pltpu.VMEM((6, half, plane), BF16),
            pltpu.VMEM((2, 6, half, plane), BF16),
            pltpu.VMEM((6, plane // 128, n, 128), F32),
            pltpu.VMEM((6, plane // 128, n, 128), F32),
            pltpu.VMEM((4, 768, 256), BF16),
            pltpu.VMEM((4, 4 * cols, 768), BF16),
            pltpu.VMEM((4, 4 * cols, 768), BF16),
            pltpu.VMEM((4 * cols, 256), F32),
            pltpu.VMEM((nq, 4, packed, 128), BF16),
            pltpu.VMEM((nq, 2, packed, 128), BF16),
            pltpu.VMEM((nq, 2, packed, 128), BF16),
            pltpu.VMEM((nq, packed, 128), BF16),
            pltpu.VMEM((nq, packed, 128), BF16),
            pltpu.VMEM((nq, 2, packed, 128), BF16),
            pltpu.VMEM((nq, packed, 128), BF16),
            pltpu.VMEM((SIDE, SIDE, packed, 128), BF16),
            pltpu.VMEM((SIDE, packed, 128), F32),
            pltpu.VMEM((SIDE, packed, 128), F32),
            pltpu.VMEM((SIDE, packed, 128), F32),
            dma((2,)), dma((2,)), dma((2,)), dma((2,)),
            dma((nq, 2)), dma((nq, 2)), dma((nq,)), dma((nq,)),
            dma((nq, 2)), dma((nq, 2)), dma((nq,)), dma((SIDE, SIDE)), dma((SIDE,)), dma((SIDE,)),
        ],
        compiler_params=pltpu.CompilerParams(
            collective_id=0, has_side_effects=True, vmem_limit_bytes=60 * 1024 * 1024
        ),
    )(weights, fields, link_rows, phase, mix, left)
    return out[:, :n].reshape(cols, 2, half).transpose(1, 2, 0)


def solution(mesh):
    split = Mesh(
        mesh.devices.reshape(mesh.shape["groups"], NX, NZ, mesh.shape["ea"]),
        ("groups", "gz_0", "gz_1", "ea"),
    )
    in_specs = (
        P("ea", None, None, GROUPS_GZ, None),
        P(None, None, None, None, GROUPS_GZ, None),
        P("groups"),
        P("groups"),
        P("groups", None),
        P("groups", None, None, None, None),
    )
    out_specs = P("groups", "ea", GZ)
    return jax.shard_map(
        shards, mesh=split, in_specs=in_specs, out_specs=out_specs, check_vma=False
    )
```

```python
import functools
import math

import jax
import jax.numpy as jnp
from jax import lax
from jax.experimental import pallas as pl
from jax.experimental.pallas import tpu as pltpu
from jax.sharding import Mesh
from jax.sharding import PartitionSpec as P

LX = 32
LY = 16
NX = 4
NZ = 16
SIDE = 2
GZ = ("gz_0", "gz_1")
GROUPS_GZ = ("groups", "gz_0", "gz_1")
MESH = pl.DeviceIdType.MESH
F32 = jnp.float32
BF16 = jnp.bfloat16


def prepare(half, scale, sizes, ea, along_z, spins, moms, pbuf, mix_ref, left_ref, phase_ref):
    def split(ref, at, value):
        high = value.astype(BF16)
        ref[0, at, :] = high
        ref[1, at, :] = (value - high.astype(F32)).astype(BF16)

    n = pbuf.shape[-1]

    def block(q, part):
        return pbuf[spins[0, q], spins[1, q], part].T

    for slot, q in ((0, 1), (1, 2)):
        re, im = block(q, 0), block(q, 1)
        split(mix_ref.at[slot], slice(0, n), jnp.concatenate([re, -im], 1))
        split(mix_ref.at[slot], slice(n, 2 * n), jnp.concatenate([im, re], 1))
    re = block(0, 0) * scale
    im = block(0, 1) * scale
    first = ea == 0
    pad = jnp.zeros((128 - 2 * half, 2 * n), F32)
    for own in range(2):
        low, high = slice(0, half), slice(half, 2 * half)
        one, two = (low, high) if own == 0 else (high, low)
        r = jnp.where(first, re[one], re[two])
        i = jnp.where(first, im[one], im[two])
        real = jnp.concatenate([r, -i], 1)
        imag = jnp.concatenate([i, r], 1)
        split(left_ref.at[0], slice(own * 128, own * 128 + 128), jnp.concatenate([real, imag, pad], 0))
        split(left_ref.at[1], slice(own * 128, own * 128 + 128), jnp.concatenate([-imag, real, pad], 0))
    lx, ly, depth = sizes
    sites = lax.broadcasted_iota(jnp.int32, (8, lx * ly), 1)
    xcoord = lax.rem(sites, lx)
    ycoord = lax.div(sites, lx)
    two_pi = 2.0 * math.pi
    inplane = (moms[0] * xcoord).astype(F32) / lx + (moms[1] * ycoord).astype(F32) / ly
    along = jnp.full((8, lx * ly), moms[2] * along_z, jnp.int32).astype(F32)
    angle = two_pi * inplane + two_pi * along / depth
    phase_ref[0] = jnp.cos(angle)
    phase_ref[1] = jnp.sin(angle)


def times(lr, li, vr, vi):
    return lr * vr - li * vi, lr * vi + li * vr


def times_conj(lr, li, vr, vi):
    return lr * vr + li * vi, lr * vi - li * vr


def main_kernel(
    scale, weights, spins, moms, v_ref, links, peram, out_ref,
    pbuf, phase, mix, left,
    vall, upper, lower, back, disp, phown, phall, v1, v2, lmat, wbuf0, wbuf1, acc,
    grid_in, mine, grid_out, far_in, mid_out, x_in, near_out, near_in, near_own, ring_out, plus_in, minus_in,
    p_sem, halo_s, halo_r, ea_s, ea_r, dd_s, dd_r, fx_s, fx_r, x_s, x_r, near_s, near_r, plus_s, plus_r, minus_s, minus_r,
):
    ncomp, half, plane = v_ref.shape
    cols = out_ref.shape[0]
    packed = far_in.shape[1]
    tiles = cols // 16
    per_row = 2 * half // 16
    x = lax.axis_index("gz_0")
    z = lax.axis_index("gz_1")
    e = lax.axis_index("ea")
    nx = lax.axis_size("gz_0")
    nz = lax.axis_size("gz_1")
    sgn = 1 - 2 * e
    xp = lax.rem(x + sgn + nx, nx)
    xm = lax.rem(x - sgn + nx, nx)
    zh = z // SIDE
    zl = lax.rem(z, SIDE)
    partner = {"ea": 1 - e}
    to_xp = {"gz_0": xp}
    to_xm = {"gz_0": xm}
    gz = x * nz + z
    gup = lax.rem(gz + 1, nx * nz)
    gdn = lax.rem(gz + nx * nz - 1, nx * nz)
    site_up = {"gz_0": gup // nz, "gz_1": lax.rem(gup, nz)}
    site_dn = {"gz_0": gdn // nz, "gz_1": lax.rem(gdn, nz)}

    nh = nz // SIDE
    pair = {"gz_1": zh * SIDE + 1 - zl}
    ring_up = {"gz_1": lax.rem(zh + 1, nh) * SIDE + zl}
    ring_dn = {"gz_1": lax.rem(zh + nh - 1, nh) * SIDE + zl}
    ring = 4

    def remote(src, dst, s, r, to):
        return pltpu.make_async_remote_copy(
            src_ref=src, dst_ref=dst, send_sem=s, recv_sem=r, device_id=to, device_id_type=MESH
        )

    barrier = pltpu.get_barrier_semaphore()
    peers = [partner, to_xp, to_xm, site_up, site_dn]
    peers += [pair, ring_up, ring_dn]
    for to in peers:
        pl.semaphore_signal(barrier, inc=1, device_id=to, device_id_type=MESH)
    pl.semaphore_wait(barrier, len(peers))

    rows = 16
    chunks = half // rows

    def chunk_of(ref, t):
        return ref.at[:, pl.ds(t * rows, rows), :]

    def v_copy(t):
        return remote(
            chunk_of(v_ref, t), chunk_of(upper, t), halo_s.at[0, t], halo_r.at[0, t], site_dn
        )

    def b_copy(t):
        return remote(
            chunk_of(back, t), chunk_of(lower, t), halo_s.at[1, t], halo_r.at[1, t], site_up
        )

    def ph_copy(t):
        return remote(
            chunk_of(phown, t), chunk_of(phall.at[e], t), ea_s.at[1 + t], ea_r.at[1 + t], partner
        )

    for t in range(chunks):
        v_copy(t).start()
    fetch = pltpu.make_async_copy(peram, pbuf, p_sem)
    fetch.start()
    send_ea = remote(v_ref, vall.at[e], ea_s.at[0], ea_r.at[0], partner)
    send_ea.start()

    def field(ref, r0):
        return [ref[c, pl.ds(r0, rows), :].astype(F32) for c in range(ncomp)]

    def link(d, row, col, part):
        return links[((d * 3 + row) * 3 + col) * 2 + part]

    def apply(d, f):
        out = []
        for row in range(3):
            re, im = 0.0, 0.0
            for col in range(3):
                a, b = times(link(d, row, col, 0), link(d, row, col, 1), f[2 * col], f[2 * col + 1])
                re, im = re + a, im + b
            out += [re, im]
        return out

    def adjoint(d, f):
        out = []
        for col in range(3):
            re, im = 0.0, 0.0
            for row in range(3):
                a, b = times_conj(
                    link(d, row, col, 0), link(d, row, col, 1), f[2 * row], f[2 * row + 1]
                )
                re, im = re + a, im + b
            out += [re, im]
        return out

    def back_tile(t):
        r0 = t * rows
        f = field(v_ref, r0)
        for c, val in enumerate(adjoint(2, f)):
            back[c, pl.ds(r0, rows), :] = val.astype(BF16)
        for c in range(ncomp):
            vall[e, c, pl.ds(r0, rows), :] = v_ref[c, pl.ds(r0, rows), :]

    for t in range(chunks):
        back_tile(t)
        b_copy(t).start()
    fetch.wait()
    prepare(half, scale, (LX, LY, nx * nz), e, gz, spins, moms, pbuf, mix, left, phase)

    lane = lax.broadcasted_iota(jnp.int32, (rows, plane), 1)
    xc = lax.rem(lane, LX)

    def shift_x(val, by):
        if by < 0:
            return jnp.where(
                xc == LX - 1, pltpu.roll(val, LX - 1, 1), pltpu.roll(val, plane - 1, 1)
            )
        return jnp.where(xc == 0, pltpu.roll(val, plane - (LX - 1), 1), pltpu.roll(val, 1, 1))

    def shift_y(val, by):
        return pltpu.roll(val, plane - LX if by < 0 else LX, 1)

    def inplane_tile(t, _):
        r0 = pl.multiple_of(t * rows, rows)
        for d, shift in ((0, shift_x), (1, shift_y)):
            f = field(v_ref, r0)
            ahead = apply(d, [shift(c, -1) for c in f])
            behind = [shift(c.astype(BF16).astype(F32), 1) for c in adjoint(d, f)]
            for c in range(ncomp):
                term = weights[d].astype(F32) * (ahead[c] - behind[c])
                if d == 0:
                    disp[c, pl.ds(r0, rows), :] = term
                else:
                    disp[c, pl.ds(r0, rows), :] += term
        return 0

    send_ea.wait()
    for slot, dst in ((0, v1), (1, v2)):
        for k in range(3):
            stack = jnp.concatenate(
                [vall[0, 2 * k], vall[1, 2 * k], vall[0, 2 * k + 1], vall[1, 2 * k + 1]], 0
            )
            res = jnp.dot(mix[slot, 0], stack, preferred_element_type=F32) + jnp.dot(
                mix[slot, 1], stack, preferred_element_type=F32
            )
            for r in range(2):
                part = res[2 * half * r : 2 * half * (r + 1)]
                for lt in range(plane // 128):
                    dst[2 * k + r, lt] = part[:, lt * 128 : lt * 128 + 128]

    def dest_z(q):
        step = q // 2
        hop = step // 2
        to = jnp.where(lax.rem(step, 2) == 0, zh + ring - hop, zh + 1 - ring + hop + nh)
        return lax.rem(to, nh) * SIDE + jnp.where(lax.rem(q, 2) == 0, 1 - zl, zl)

    turns = 4

    def w_section(dst, step, sec):
        par = sec // 2
        blk = sec - 2 * par
        xd = lax.rem(jnp.where(blk == 0, x + sgn + nx, x + 2 * (1 - e)), nx)
        first = (xd * nz + dest_z(2 * step + par)) * tiles
        row = first // per_row
        skip = first - row * per_row
        for t in range(tiles):
            u = skip + t
            over = jnp.where(u >= per_row, 1, 0) + jnp.where(u >= 2 * per_row, 1, 0)
            b2 = row + over
            c0 = pl.multiple_of((u - over * per_row) * 16, 16)
            row0 = pl.multiple_of(sec * cols + t * 16, 16)
            for lt in range(plane // 128):
                b = [v1[c, lt, pl.ds(b2, 16, stride=0), :] for c in range(ncomp)]
                w = [v2[c, lt, pl.ds(c0, 16), :] for c in range(ncomp)]
                for k, (i, j) in enumerate(((1, 2), (2, 0), (0, 1))):
                    ar, ai, br, bi = b[2 * i], b[2 * i + 1], b[2 * j], b[2 * j + 1]
                    cr, ci, dr, di = w[2 * i], w[2 * i + 1], w[2 * j], w[2 * j + 1]
                    re = ar * dr - ai * di - (br * cr - bi * ci)
                    im = ar * di + ai * dr - (br * ci + bi * cr)
                    for r, val in ((0, re), (1, im)):
                        piece = 2 * (2 * k + r) + lt // 2
                        at = (piece % 3) * 256 + (lt % 2) * 128
                        dst[piece // 3, pl.ds(row0, 16), at : at + 128] = val.astype(BF16)

    def w_only(dst, step):
        lax.fori_loop(0, turns, lambda k, c: (w_section(dst, step, k), 0)[1], 0)

    def dot_turn(src, k):
        acc[...] += jnp.dot(src[k], lmat[k], preferred_element_type=F32)

    def fused(src, dst, step):
        acc[...] = jnp.zeros_like(acc)

        def turn(k, _):
            dot_turn(src, k)
            w_section(dst, step + 1, k)
            return 0

        lax.fori_loop(0, turns, turn, 0)

    def dot_only(src):
        acc[...] = jnp.zeros_like(acc)
        lax.fori_loop(0, turns, lambda k, c: (dot_turn(src, k), 0)[1], 0)

    def to_partner(q, blk):
        role = 1 if blk == 0 else 2 + e
        return remote(
            grid_out.at[q, blk], grid_in.at[q, role], dd_s.at[q, blk], dd_r.at[q, blk], partner
        )

    fill = lax.broadcasted_iota(jnp.int32, (32, 128), 1) < 2 * half

    def pack(rows_at, lanes):
        for g in range(3):
            extra = acc[rows_at + packed : rows_at + cols, lanes]
            extra = pltpu.roll(extra, 2 * half - 32 * g, 1)
            yield jnp.where(fill, acc[rows_at + 32 * g : rows_at + 32 * g + 32, lanes], extra)
        yield acc[rows_at + 96 : rows_at + packed, lanes]

    def put(ref, pieces):
        at = 0
        for piece in pieces:
            ref[at : at + piece.shape[0], :] = piece.astype(BF16)
            at += piece.shape[0]

    def give(step):
        for par in range(2):
            for blk in range(2):
                q = 2 * step + par
                rows_at = (2 * par + blk) * cols
                put(grid_out.at[q, blk], pack(rows_at, slice(128, 256)))
                to_partner(q, blk).start()
                put(mine.at[q, blk], pack(rows_at, slice(0, 128)))

    def far_copy(q):
        return remote(grid_in.at[q, 2], far_in.at[q], fx_s.at[q], fx_r.at[q], to_xp)

    def far_mine(q):
        return remote(mine.at[q, 1], far_in.at[q], fx_s.at[q], fx_r.at[q], to_xp)

    def direct_copy(q):
        return remote(grid_in.at[q, 1], x_in.at[q, 0], x_s.at[q, 0], x_r.at[q, 0], to_xm)

    def mid_copy(q):
        return remote(mid_out.at[q], x_in.at[q, 1], x_s.at[q, 1], x_r.at[q, 1], to_xp)

    def first_x(q):
        to_partner(q, 0).wait_recv()
        to_partner(q, 1).wait_recv()

        @pl.when(e == 0)
        def _():
            far_mine(q).start()

        @pl.when(e == 1)
        def _():
            far_copy(q).start()

        direct_copy(q).start()

    def second_x(q):
        far_mine(q).wait_recv()
        mid_out[q] = (mine[q, 0].astype(F32) + far_in[q].astype(F32)).astype(BF16)
        mid_copy(q).start()

    def x_sum(q):
        direct_copy(q).wait_recv()
        mid_copy(q).wait_recv()
        total = x_in[q, 0].astype(F32) + x_in[q, 1].astype(F32)
        own = jnp.where(e == 0, grid_in[q, 3].astype(F32), mine[q, 1].astype(F32))
        return total + own

    last = 7

    def near_copy(step):
        return remote(near_out.at[step], near_in.at[step], near_s.at[step], near_r.at[step], pair)

    def near_sum(step):
        near_out[step] = x_sum(2 * step).astype(BF16)
        near_copy(step).start()
        near_own[step] = x_sum(2 * step + 1)

    def plus_copy(hop):
        return remote(
            ring_out.at[0, hop], plus_in.at[hop], plus_s.at[hop], plus_r.at[hop], ring_up
        )

    def minus_copy(hop):
        return remote(
            ring_out.at[1, hop], minus_in.at[hop], minus_s.at[hop], minus_r.at[hop], ring_dn
        )

    def ring_step(side, hop):
        step = 2 * hop + side
        copy, arrived = ((plus_copy, plus_in), (minus_copy, minus_in))[side]
        near_copy(step).wait_recv()
        ring_out[side, hop] = near_own[step] + near_in[step].astype(F32)

        @pl.when(hop > 0)
        def _():
            copy(hop - 1).wait_recv()
            ring_out[side, hop] += arrived[hop - 1]

        if side == 0:
            copy(hop).start()
        else:

            @pl.when(hop < ring - 1)
            def _():
                copy(hop).start()

    w_only(wbuf0, 0)
    lax.fori_loop(0, half // rows, inplane_tile, 0)
    cosine = phase[0, 0:1]
    sine = phase[1, 0:1]

    def zdir_tile(t):
        r0 = t * rows
        ahead = apply(2, field(upper, r0))
        low = field(lower, r0)
        tot = [
            disp[c, pl.ds(r0, rows), :] + weights[2].astype(F32) * (ahead[c] - low[c])
            for c in range(ncomp)
        ]
        for k in range(3):
            re, im = tot[2 * k], tot[2 * k + 1]
            phown[2 * k, pl.ds(r0, rows), :] = (cosine * re + sine * im).astype(BF16)
            phown[2 * k + 1, pl.ds(r0, rows), :] = (cosine * im - sine * re).astype(BF16)
        for c in range(ncomp):
            phall[e, c, pl.ds(r0, rows), :] = phown[c, pl.ds(r0, rows), :]

    for t in range(chunks):
        v_copy(t).wait_recv()
        b_copy(t).wait_recv()
        zdir_tile(t)
        ph_copy(t).start()
    for t in range(chunks):
        ph_copy(t).wait_recv()
    for k in range(3):
        stack = jnp.concatenate(
            [phall[0, 2 * k], phall[1, 2 * k], phall[0, 2 * k + 1], phall[1, 2 * k + 1]], 0
        )
        for r in range(2):
            res = jnp.dot(left[r, 0], stack, preferred_element_type=F32) + jnp.dot(
                left[r, 1], stack, preferred_element_type=F32
            )
            turned = res.T.astype(BF16)
            for hf in range(2):
                piece = 2 * (2 * k + r) + hf
                at = (piece % 3) * 256
                lmat[piece // 3, at : at + 256, :] = turned[hf * 256 : hf * 256 + 256]

    def stage(step, src, dst):
        @pl.when(step < last)
        def _():
            fused(src, dst, step)

        @pl.when(step == last)
        def _():
            dot_only(src)

        @pl.when((step >= 1) & (step <= last + 1))
        def _():
            first_x(2 * (step - 1))
            first_x(2 * (step - 1) + 1)

        @pl.when(step <= last)
        def _():
            give(step)

        @pl.when((step >= 3) & (step <= last + 3))
        def _():
            second_x(2 * (step - 3))
            second_x(2 * (step - 3) + 1)

        @pl.when((step >= 5) & (step <= last + 5))
        def _():
            near_sum(step - 5)

    def body(i, _):
        stage(2 * i, wbuf0, wbuf1)

        @pl.when(i >= 4)
        def _():
            ring_step(1, i - 4)

        stage(2 * i + 1, wbuf1, wbuf0)

        @pl.when((i >= 3) & (i <= 6))
        def _():
            ring_step(0, i - 3)

        return 0

    lax.fori_loop(0, 8, body, 0)
    plus_copy(ring - 1).wait_recv()
    total = ring_out[1, ring - 1] + plus_in[ring - 1]
    out_ref[0:packed, :] = total
    spot = lax.broadcasted_iota(jnp.int32, (32, 128), 1)
    extra = jnp.zeros((32, 128), F32)
    for g in range(3):
        piece = pltpu.roll(total[32 * g : 32 * g + 32], (128 - 2 * half + 32 * g) % 128, 1)
        extra = jnp.where((spot >= 32 * g) & (spot < 32 * g + 32), piece, extra)
    out_ref[packed:cols, :] = extra

    def drain(q, _):
        to_partner(q, 0).wait_send()
        to_partner(q, 1).wait_send()
        far_mine(q).wait_send()
        direct_copy(q).wait_send()
        mid_copy(q).wait_send()

        return 0

    lax.fori_loop(0, 2 * (last + 1), drain, 0)
    for t in range(chunks):
        v_copy(t).wait_send()
        b_copy(t).wait_send()
        ph_copy(t).wait_send()
    for step in range(last + 1):
        near_copy(step).wait_send()
    for hop in range(ring):
        plus_copy(hop).wait_send()
        if hop < ring - 1:
            minus_copy(hop).wait_send()


def shards(eigvec, links, momentum, weights, spins, peram):
    half = eigvec.shape[0]
    plane = eigvec.shape[4]
    n = 2 * half
    nx, nz, cores = lax.axis_size("gz_0"), lax.axis_size("gz_1"), lax.axis_size("ea")
    depth = nx * nz
    cols = n * n // depth
    scale = 1.0 / math.sqrt(LX * LY * depth)
    fields = eigvec.reshape(half, 6, plane).transpose(1, 0, 2)
    link_rows = links.reshape(54, 1, plane)
    vm = pl.BlockSpec(memory_space=pltpu.VMEM)
    dma = pltpu.SemaphoreType.DMA
    nq = nz
    packed = cols - 32
    out = pl.pallas_call(
        functools.partial(main_kernel, scale),
        out_shape=jax.ShapeDtypeStruct((cols, 128), F32),
        in_specs=[pl.BlockSpec(memory_space=pltpu.SMEM)] * 3 + [vm] * 2 + [pl.BlockSpec(memory_space=pl.ANY)],
        out_specs=vm,
        scratch_shapes=[
            pltpu.VMEM(peram.shape, F32),
            pltpu.VMEM((2, 8, plane), F32),
            pltpu.VMEM((2, 2, 2 * n, 2 * n), BF16),
            pltpu.VMEM((2, 2, 256, 2 * n), BF16),
            pltpu.VMEM((2, 6, half, plane), BF16),
            pltpu.VMEM((6, half, plane), BF16),
            pltpu.VMEM((6, half, plane), BF16),
            pltpu.VMEM((6, half, plane), BF16),
            pltpu.VMEM((6, half, plane), F32),
            pltpu.VMEM((6, half, plane), BF16),
            pltpu.VMEM((2, 6, half, plane), BF16),
            pltpu.VMEM((6, plane // 128, n, 128), F32),
            pltpu.VMEM((6, plane // 128, n, 128), F32),
            pltpu.VMEM((4, 768, 256), BF16),
            pltpu.VMEM((4, 4 * cols, 768), BF16),
            pltpu.VMEM((4, 4 * cols, 768), BF16),
            pltpu.VMEM((4 * cols, 256), F32),
            pltpu.VMEM((nq, 4, packed, 128), BF16),
            pltpu.VMEM((nq, 2, packed, 128), BF16),
            pltpu.VMEM((nq, 2, packed, 128), BF16),
            pltpu.VMEM((nq, packed, 128), BF16),
            pltpu.VMEM((nq, packed, 128), BF16),
            pltpu.VMEM((nq, 2, packed, 128), BF16),
            pltpu.VMEM((8, packed, 128), BF16),
            pltpu.VMEM((8, packed, 128), BF16),
            pltpu.VMEM((8, packed, 128), F32),
            pltpu.VMEM((2, 4, packed, 128), F32),
            pltpu.VMEM((4, packed, 128), F32),
            pltpu.VMEM((4, packed, 128), F32),
            dma, dma((2, 3)), dma((2, 3)), dma((4,)), dma((4,)),
            dma((nq, 2)), dma((nq, 2)), dma((nq,)), dma((nq,)),
            dma((nq, 2)), dma((nq, 2)), dma((8,)), dma((8,)), dma((4,)), dma((4,)), dma((4,)), dma((4,)),
        ],
        compiler_params=pltpu.CompilerParams(
            collective_id=0, has_side_effects=True, vmem_limit_bytes=60 * 1024 * 1024
        ),
    )(weights, spins.T, momentum, fields, link_rows, peram)
    return out[:, :n].reshape(cols, 2, half).transpose(1, 2, 0)


def solution(mesh):
    split = Mesh(
        mesh.devices.reshape(mesh.shape["groups"], NX, NZ, mesh.shape["ea"]),
        ("groups", "gz_0", "gz_1", "ea"),
    )
    in_specs = (
        P("ea", None, None, GROUPS_GZ, None),
        P(None, None, None, None, GROUPS_GZ, None),
        P("groups"),
        P("groups"),
        P("groups", None),
        P("groups", None, None, None, None),
    )
    out_specs = P("groups", "ea", GZ)
    return jax.shard_map(
        shards, mesh=split, in_specs=in_specs, out_specs=out_specs, check_vma=False
    )
```

```python
import functools
import math

import jax
import jax.numpy as jnp
from jax import lax
from jax.experimental import pallas as pl
from jax.experimental.pallas import tpu as pltpu
from jax.sharding import Mesh
from jax.sharding import PartitionSpec as P

LX = 32
LY = 16
NX = 4
NZ = 16
SIDE = 2
GZ = ("gz_0", "gz_1")
GROUPS_GZ = ("groups", "gz_0", "gz_1")
MESH = pl.DeviceIdType.MESH
F32 = jnp.float32
BF16 = jnp.bfloat16


def prepare(half, scale, sizes, ea, along_z, spins, moms, pbuf, mix_ref, left_ref, phase_ref):
    def split(ref, at, value):
        high = value.astype(BF16)
        ref[0, at, :] = high
        ref[1, at, :] = (value - high.astype(F32)).astype(BF16)

    n = pbuf.shape[-1]

    def block(q, part):
        return pbuf[spins[0, q], spins[1, q], part].T

    for slot, q in ((0, 1), (1, 2)):
        re, im = block(q, 0), block(q, 1)
        split(mix_ref.at[slot], slice(0, n), jnp.concatenate([re, -im], 1))
        split(mix_ref.at[slot], slice(n, 2 * n), jnp.concatenate([im, re], 1))
    re = block(0, 0) * scale
    im = block(0, 1) * scale
    first = ea == 0
    pad = jnp.zeros((128 - 2 * half, 2 * n), F32)
    for own in range(2):
        low, high = slice(0, half), slice(half, 2 * half)
        one, two = (low, high) if own == 0 else (high, low)
        r = jnp.where(first, re[one], re[two])
        i = jnp.where(first, im[one], im[two])
        real = jnp.concatenate([r, -i], 1)
        imag = jnp.concatenate([i, r], 1)
        split(left_ref.at[0], slice(own * 128, own * 128 + 128), jnp.concatenate([real, imag, pad], 0))
        split(left_ref.at[1], slice(own * 128, own * 128 + 128), jnp.concatenate([-imag, real, pad], 0))
    lx, ly, depth = sizes
    sites = lax.broadcasted_iota(jnp.int32, (8, lx * ly), 1)
    xcoord = lax.rem(sites, lx)
    ycoord = lax.div(sites, lx)
    two_pi = 2.0 * math.pi
    inplane = (moms[0] * xcoord).astype(F32) / lx + (moms[1] * ycoord).astype(F32) / ly
    along = jnp.full((8, lx * ly), moms[2] * along_z, jnp.int32).astype(F32)
    angle = two_pi * inplane + two_pi * along / depth
    phase_ref[0] = jnp.cos(angle)
    phase_ref[1] = jnp.sin(angle)


def times(lr, li, vr, vi):
    return lr * vr - li * vi, lr * vi + li * vr


def times_conj(lr, li, vr, vi):
    return lr * vr + li * vi, lr * vi - li * vr


def main_kernel(
    scale, weights, spins, moms, v_ref, links, peram, out_ref,
    pbuf, phase, mix, left,
    vall, upper, lower, back, disp, phown, phall, v1, v2, lmat, wbuf0, wbuf1, acc,
    grid_in, mine, grid_out, far_in, mid_out, x_in, near_out, near_in, near_own, ring_out, plus_in, minus_in, short_out, plus_short, minus_short,
    p_sem, halo_s, halo_r, ea_s, ea_r, dd_s, dd_r, fx_s, fx_r, x_s, x_r, near_s, near_r, plus_s, plus_r, minus_s, minus_r,
):
    ncomp, half, plane = v_ref.shape
    cols = out_ref.shape[0]
    packed = far_in.shape[1]
    tiles = cols // 16
    per_row = 2 * half // 16
    x = lax.axis_index("gz_0")
    z = lax.axis_index("gz_1")
    e = lax.axis_index("ea")
    nx = lax.axis_size("gz_0")
    nz = lax.axis_size("gz_1")
    sgn = 1 - 2 * e
    xp = lax.rem(x + sgn + nx, nx)
    xm = lax.rem(x - sgn + nx, nx)
    zh = z // SIDE
    zl = lax.rem(z, SIDE)
    partner = {"ea": 1 - e}
    to_xp = {"gz_0": xp}
    to_xm = {"gz_0": xm}
    gz = x * nz + z
    gup = lax.rem(gz + 1, nx * nz)
    gdn = lax.rem(gz + nx * nz - 1, nx * nz)
    site_up = {"gz_0": gup // nz, "gz_1": lax.rem(gup, nz)}
    site_dn = {"gz_0": gdn // nz, "gz_1": lax.rem(gdn, nz)}

    nh = nz // SIDE
    pair = {"gz_1": zh * SIDE + 1 - zl}
    ring_up = {"gz_1": lax.rem(zh + 1, nh) * SIDE + zl}
    ring_dn = {"gz_1": lax.rem(zh + nh - 1, nh) * SIDE + zl}
    ring = 4

    def remote(src, dst, s, r, to):
        return pltpu.make_async_remote_copy(
            src_ref=src, dst_ref=dst, send_sem=s, recv_sem=r, device_id=to, device_id_type=MESH
        )

    barrier = pltpu.get_barrier_semaphore()
    peers = [partner, to_xp, to_xm, site_up, site_dn]
    peers += [pair, ring_up, ring_dn]
    for to in peers:
        pl.semaphore_signal(barrier, inc=1, device_id=to, device_id_type=MESH)
    pl.semaphore_wait(barrier, len(peers))

    rows = 16
    chunks = half // rows

    def chunk_of(ref, t):
        return ref.at[:, pl.ds(t * rows, rows), :]

    def v_copy(t):
        return remote(
            chunk_of(v_ref, t), chunk_of(upper, t), halo_s.at[0, t], halo_r.at[0, t], site_dn
        )

    def b_copy(t):
        return remote(
            chunk_of(back, t), chunk_of(lower, t), halo_s.at[1, t], halo_r.at[1, t], site_up
        )

    def ph_copy(t):
        return remote(
            chunk_of(phown, t), chunk_of(phall.at[e], t), ea_s.at[1 + t], ea_r.at[1 + t], partner
        )

    for t in range(chunks):
        v_copy(t).start()
    fetch = pltpu.make_async_copy(peram, pbuf, p_sem)
    fetch.start()
    send_ea = remote(v_ref, vall.at[e], ea_s.at[0], ea_r.at[0], partner)
    send_ea.start()

    def field(ref, r0):
        return [ref[c, pl.ds(r0, rows), :].astype(F32) for c in range(ncomp)]

    def link(d, row, col, part):
        return links[((d * 3 + row) * 3 + col) * 2 + part]

    def apply(d, f):
        out = []
        for row in range(3):
            re, im = 0.0, 0.0
            for col in range(3):
                a, b = times(link(d, row, col, 0), link(d, row, col, 1), f[2 * col], f[2 * col + 1])
                re, im = re + a, im + b
            out += [re, im]
        return out

    def adjoint(d, f):
        out = []
        for col in range(3):
            re, im = 0.0, 0.0
            for row in range(3):
                a, b = times_conj(
                    link(d, row, col, 0), link(d, row, col, 1), f[2 * row], f[2 * row + 1]
                )
                re, im = re + a, im + b
            out += [re, im]
        return out

    def back_tile(t):
        r0 = t * rows
        f = field(v_ref, r0)
        for c, val in enumerate(adjoint(2, f)):
            back[c, pl.ds(r0, rows), :] = val.astype(BF16)
        for c in range(ncomp):
            vall[e, c, pl.ds(r0, rows), :] = v_ref[c, pl.ds(r0, rows), :]

    for t in range(chunks):
        back_tile(t)
        b_copy(t).start()
    fetch.wait()
    prepare(half, scale, (LX, LY, nx * nz), e, gz, spins, moms, pbuf, mix, left, phase)

    lane = lax.broadcasted_iota(jnp.int32, (rows, plane), 1)
    xc = lax.rem(lane, LX)

    def shift_x(val, by):
        if by < 0:
            return jnp.where(
                xc == LX - 1, pltpu.roll(val, LX - 1, 1), pltpu.roll(val, plane - 1, 1)
            )
        return jnp.where(xc == 0, pltpu.roll(val, plane - (LX - 1), 1), pltpu.roll(val, 1, 1))

    def shift_y(val, by):
        return pltpu.roll(val, plane - LX if by < 0 else LX, 1)

    def inplane_tile(t, _):
        r0 = pl.multiple_of(t * rows, rows)
        for d, shift in ((0, shift_x), (1, shift_y)):
            f = field(v_ref, r0)
            ahead = apply(d, [shift(c, -1) for c in f])
            behind = [shift(c.astype(BF16).astype(F32), 1) for c in adjoint(d, f)]
            for c in range(ncomp):
                term = weights[d].astype(F32) * (ahead[c] - behind[c])
                if d == 0:
                    disp[c, pl.ds(r0, rows), :] = term
                else:
                    disp[c, pl.ds(r0, rows), :] += term
        return 0

    send_ea.wait()
    for slot, dst in ((0, v1), (1, v2)):
        for k in range(3):
            stack = jnp.concatenate(
                [vall[0, 2 * k], vall[1, 2 * k], vall[0, 2 * k + 1], vall[1, 2 * k + 1]], 0
            )
            res = jnp.dot(mix[slot, 0], stack, preferred_element_type=F32) + jnp.dot(
                mix[slot, 1], stack, preferred_element_type=F32
            )
            for r in range(2):
                part = res[2 * half * r : 2 * half * (r + 1)]
                for lt in range(plane // 128):
                    dst[2 * k + r, lt] = part[:, lt * 128 : lt * 128 + 128]

    def dest_z(q):
        step = q // 2
        hop = step // 2
        to = jnp.where(lax.rem(step, 2) == 0, zh + ring - hop, zh + 1 - ring + hop + nh)
        return lax.rem(to, nh) * SIDE + jnp.where(lax.rem(q, 2) == 0, 1 - zl, zl)

    turns = 4

    def w_section(dst, step, sec):
        par = sec // 2
        blk = sec - 2 * par
        xd = lax.rem(jnp.where(blk == 0, x + sgn + nx, x + 2 * (1 - e)), nx)
        first = (xd * nz + dest_z(2 * step + par)) * tiles
        row = first // per_row
        skip = first - row * per_row
        for t in range(tiles):
            u = skip + t
            over = jnp.where(u >= per_row, 1, 0) + jnp.where(u >= 2 * per_row, 1, 0)
            b2 = row + over
            c0 = pl.multiple_of((u - over * per_row) * 16, 16)
            row0 = pl.multiple_of(sec * cols + t * 16, 16)
            for lt in range(plane // 128):
                b = [v1[c, lt, pl.ds(b2, 16, stride=0), :] for c in range(ncomp)]
                w = [v2[c, lt, pl.ds(c0, 16), :] for c in range(ncomp)]
                for k, (i, j) in enumerate(((1, 2), (2, 0), (0, 1))):
                    ar, ai, br, bi = b[2 * i], b[2 * i + 1], b[2 * j], b[2 * j + 1]
                    cr, ci, dr, di = w[2 * i], w[2 * i + 1], w[2 * j], w[2 * j + 1]
                    re = ar * dr - ai * di - (br * cr - bi * ci)
                    im = ar * di + ai * dr - (br * ci + bi * cr)
                    for r, val in ((0, re), (1, im)):
                        piece = 2 * (2 * k + r) + lt // 2
                        at = (piece % 3) * 256 + (lt % 2) * 128
                        dst[piece // 3, pl.ds(row0, 16), at : at + 128] = val.astype(BF16)

    def w_only(dst, step):
        lax.fori_loop(0, turns, lambda k, c: (w_section(dst, step, k), 0)[1], 0)

    def dot_turn(src, k):
        acc[...] += jnp.dot(src[k], lmat[k], preferred_element_type=F32)

    def fused(src, dst, step, part):
        if part == 0:
            acc[...] = jnp.zeros_like(acc)

        def turn(k, _):
            dot_turn(src, k)
            w_section(dst, step + 1, k)
            return 0

        lax.fori_loop(part * 2, part * 2 + 2, turn, 0)

    def dot_only(src):
        acc[...] = jnp.zeros_like(acc)
        lax.fori_loop(0, turns, lambda k, c: (dot_turn(src, k), 0)[1], 0)

    def to_partner(q, blk):
        role = 1 if blk == 0 else 2 + e
        return remote(
            grid_out.at[q, blk], grid_in.at[q, role], dd_s.at[q, blk], dd_r.at[q, blk], partner
        )

    fill = lax.broadcasted_iota(jnp.int32, (32, 128), 1) < 2 * half

    def pack(rows_at, lanes):
        for g in range(3):
            extra = acc[rows_at + packed : rows_at + cols, lanes]
            extra = pltpu.roll(extra, 2 * half - 32 * g, 1)
            yield jnp.where(fill, acc[rows_at + 32 * g : rows_at + 32 * g + 32, lanes], extra)
        yield acc[rows_at + 96 : rows_at + packed, lanes]

    def put(ref, pieces):
        at = 0
        for piece in pieces:
            ref[at : at + piece.shape[0], :] = piece.astype(BF16)
            at += piece.shape[0]

    def give(step):
        for par in range(2):
            for blk in range(2):
                q = 2 * step + par
                rows_at = (2 * par + blk) * cols
                put(grid_out.at[q, blk], pack(rows_at, slice(128, 256)))
                to_partner(q, blk).start()
                put(mine.at[q, blk], pack(rows_at, slice(0, 128)))

    def far_copy(q):
        return remote(grid_in.at[q, 2], far_in.at[q], fx_s.at[q], fx_r.at[q], to_xp)

    def far_mine(q):
        return remote(mine.at[q, 1], far_in.at[q], fx_s.at[q], fx_r.at[q], to_xp)

    def direct_copy(q):
        return remote(grid_in.at[q, 1], x_in.at[q, 0], x_s.at[q, 0], x_r.at[q, 0], to_xm)

    def mid_copy(q):
        return remote(mid_out.at[q], x_in.at[q, 1], x_s.at[q, 1], x_r.at[q, 1], to_xp)

    def first_x(q):
        to_partner(q, 0).wait_recv()
        to_partner(q, 1).wait_recv()

        @pl.when(e == 0)
        def _():
            far_mine(q).start()

        @pl.when(e == 1)
        def _():
            far_copy(q).start()

        direct_copy(q).start()

    def second_x(q):
        far_mine(q).wait_recv()
        mid_out[q] = (mine[q, 0].astype(F32) + far_in[q].astype(F32)).astype(BF16)
        mid_copy(q).start()

    def x_sum(q):
        direct_copy(q).wait_recv()
        mid_copy(q).wait_recv()
        total = x_in[q, 0].astype(F32) + x_in[q, 1].astype(F32)
        own = jnp.where(e == 0, grid_in[q, 3].astype(F32), mine[q, 1].astype(F32))
        return total + own

    last = 7

    def near_copy(step):
        return remote(near_out.at[step], near_in.at[step], near_s.at[step], near_r.at[step], pair)

    def near_sum(step):
        near_out[step] = x_sum(2 * step).astype(BF16)
        near_copy(step).start()
        near_own[step] = x_sum(2 * step + 1)

    early = 2
    ring_s, ring_r = (plus_s, minus_s), (plus_r, minus_r)
    ring_to = (ring_up, ring_dn)
    short_in, full_in = (plus_short, minus_short), (plus_in, minus_in)

    def short_copy(side, hop):
        return remote(
            short_out.at[side, hop], short_in[side].at[hop],
            ring_s[side].at[hop], ring_r[side].at[hop], ring_to[side],
        )

    def full_copy(side, hop):
        return remote(
            ring_out.at[side, hop], full_in[side].at[hop],
            ring_s[side].at[hop], ring_r[side].at[hop], ring_to[side],
        )

    def ring_step(side, hop):
        step = 2 * hop + side
        near_copy(step).wait_recv()
        ring_out[side, hop] = near_own[step] + near_in[step].astype(F32)

        @pl.when((hop > 0) & (hop <= early))
        def _():
            short_copy(side, hop - 1).wait_recv()
            ring_out[side, hop] += short_in[side][hop - 1].astype(F32)

        @pl.when(hop > early)
        def _():
            full_copy(side, hop - 1).wait_recv()
            ring_out[side, hop] += full_in[side][hop - 1]

        @pl.when(hop < early)
        def _():
            short_out[side, hop] = ring_out[side, hop].astype(BF16)
            short_copy(side, hop).start()

        @pl.when((hop >= early) & (hop < ring - side))
        def _():
            full_copy(side, hop).start()

    w_only(wbuf0, 0)
    lax.fori_loop(0, half // rows, inplane_tile, 0)
    cosine = phase[0, 0:1]
    sine = phase[1, 0:1]

    def zdir_tile(t):
        r0 = t * rows
        ahead = apply(2, field(upper, r0))
        low = field(lower, r0)
        tot = [
            disp[c, pl.ds(r0, rows), :] + weights[2].astype(F32) * (ahead[c] - low[c])
            for c in range(ncomp)
        ]
        for k in range(3):
            re, im = tot[2 * k], tot[2 * k + 1]
            phown[2 * k, pl.ds(r0, rows), :] = (cosine * re + sine * im).astype(BF16)
            phown[2 * k + 1, pl.ds(r0, rows), :] = (cosine * im - sine * re).astype(BF16)
        for c in range(ncomp):
            phall[e, c, pl.ds(r0, rows), :] = phown[c, pl.ds(r0, rows), :]

    for t in range(chunks):
        v_copy(t).wait_recv()
        b_copy(t).wait_recv()
        zdir_tile(t)
        ph_copy(t).start()
    for t in range(chunks):
        ph_copy(t).wait_recv()
    for k in range(3):
        stack = jnp.concatenate(
            [phall[0, 2 * k], phall[1, 2 * k], phall[0, 2 * k + 1], phall[1, 2 * k + 1]], 0
        )
        for r in range(2):
            res = jnp.dot(left[r, 0], stack, preferred_element_type=F32) + jnp.dot(
                left[r, 1], stack, preferred_element_type=F32
            )
            turned = res.T.astype(BF16)
            for hf in range(2):
                piece = 2 * (2 * k + r) + hf
                at = (piece % 3) * 256
                lmat[piece // 3, at : at + 256, :] = turned[hf * 256 : hf * 256 + 256]

    def stage(step, src, dst):
        @pl.when(step < last)
        def _():
            fused(src, dst, step, 0)

        @pl.when((step >= 1) & (step <= last + 1))
        def _():
            first_x(2 * (step - 1))
            first_x(2 * (step - 1) + 1)

        @pl.when((step >= 4) & (step <= last + 4))
        def _():
            near_sum(step - 4)

        @pl.when(step < last)
        def _():
            fused(src, dst, step, 1)

        @pl.when(step == last)
        def _():
            dot_only(src)

        @pl.when(step <= last)
        def _():
            give(step)

        @pl.when((step >= 2) & (step <= last + 2))
        def _():
            second_x(2 * (step - 2))
            second_x(2 * (step - 2) + 1)

    def body(i, _):
        stage(2 * i, wbuf0, wbuf1)

        @pl.when(i >= 3)
        def _():
            ring_step(1, i - 3)

        stage(2 * i + 1, wbuf1, wbuf0)

        @pl.when((i >= 2) & (i <= 5))
        def _():
            ring_step(0, i - 2)

        return 0

    lax.fori_loop(0, 7, body, 0)
    full_copy(0, ring - 1).wait_recv()
    total = ring_out[1, ring - 1] + plus_in[ring - 1]
    out_ref[0:packed, :] = total
    spot = lax.broadcasted_iota(jnp.int32, (32, 128), 1)
    extra = jnp.zeros((32, 128), F32)
    for g in range(3):
        piece = pltpu.roll(total[32 * g : 32 * g + 32], (128 - 2 * half + 32 * g) % 128, 1)
        extra = jnp.where((spot >= 32 * g) & (spot < 32 * g + 32), piece, extra)
    out_ref[packed:cols, :] = extra

    def drain(q, _):
        to_partner(q, 0).wait_send()
        to_partner(q, 1).wait_send()
        far_mine(q).wait_send()
        direct_copy(q).wait_send()
        mid_copy(q).wait_send()

        return 0

    lax.fori_loop(0, 2 * (last + 1), drain, 0)
    for t in range(chunks):
        v_copy(t).wait_send()
        b_copy(t).wait_send()
        ph_copy(t).wait_send()
    for step in range(last + 1):
        near_copy(step).wait_send()
    for side in range(2):
        for hop in range(ring - side):
            (short_copy if hop < early else full_copy)(side, hop).wait_send()


def shards(eigvec, links, momentum, weights, spins, peram):
    half = eigvec.shape[0]
    plane = eigvec.shape[4]
    n = 2 * half
    nx, nz, cores = lax.axis_size("gz_0"), lax.axis_size("gz_1"), lax.axis_size("ea")
    depth = nx * nz
    cols = n * n // depth
    scale = 1.0 / math.sqrt(LX * LY * depth)
    fields = eigvec.reshape(half, 6, plane).transpose(1, 0, 2)
    link_rows = links.reshape(54, 1, plane)
    vm = pl.BlockSpec(memory_space=pltpu.VMEM)
    dma = pltpu.SemaphoreType.DMA
    nq = nz
    packed = cols - 32
    out = pl.pallas_call(
        functools.partial(main_kernel, scale),
        out_shape=jax.ShapeDtypeStruct((cols, 128), F32),
        in_specs=[pl.BlockSpec(memory_space=pltpu.SMEM)] * 3 + [vm] * 2 + [pl.BlockSpec(memory_space=pl.ANY)],
        out_specs=vm,
        scratch_shapes=[
            pltpu.VMEM(peram.shape, F32),
            pltpu.VMEM((2, 8, plane), F32),
            pltpu.VMEM((2, 2, 2 * n, 2 * n), BF16),
            pltpu.VMEM((2, 2, 256, 2 * n), BF16),
            pltpu.VMEM((2, 6, half, plane), BF16),
            pltpu.VMEM((6, half, plane), BF16),
            pltpu.VMEM((6, half, plane), BF16),
            pltpu.VMEM((6, half, plane), BF16),
            pltpu.VMEM((6, half, plane), F32),
            pltpu.VMEM((6, half, plane), BF16),
            pltpu.VMEM((2, 6, half, plane), BF16),
            pltpu.VMEM((6, plane // 128, n, 128), F32),
            pltpu.VMEM((6, plane // 128, n, 128), F32),
            pltpu.VMEM((4, 768, 256), BF16),
            pltpu.VMEM((4, 4 * cols, 768), BF16),
            pltpu.VMEM((4, 4 * cols, 768), BF16),
            pltpu.VMEM((4 * cols, 256), F32),
            pltpu.VMEM((nq, 4, packed, 128), BF16),
            pltpu.VMEM((nq, 2, packed, 128), BF16),
            pltpu.VMEM((nq, 2, packed, 128), BF16),
            pltpu.VMEM((nq, packed, 128), BF16),
            pltpu.VMEM((nq, packed, 128), BF16),
            pltpu.VMEM((nq, 2, packed, 128), BF16),
            pltpu.VMEM((8, packed, 128), BF16),
            pltpu.VMEM((8, packed, 128), BF16),
            pltpu.VMEM((8, packed, 128), F32),
            pltpu.VMEM((2, 4, packed, 128), F32),
            pltpu.VMEM((4, packed, 128), F32),
            pltpu.VMEM((4, packed, 128), F32),
            pltpu.VMEM((2, 2, packed, 128), BF16),
            pltpu.VMEM((2, packed, 128), BF16),
            pltpu.VMEM((2, packed, 128), BF16),
            dma, dma((2, 3)), dma((2, 3)), dma((4,)), dma((4,)),
            dma((nq, 2)), dma((nq, 2)), dma((nq,)), dma((nq,)),
            dma((nq, 2)), dma((nq, 2)), dma((8,)), dma((8,)), dma((4,)), dma((4,)), dma((4,)), dma((4,)),
        ],
        compiler_params=pltpu.CompilerParams(
            collective_id=0, has_side_effects=True, vmem_limit_bytes=60 * 1024 * 1024
        ),
    )(weights, spins.T, momentum, fields, link_rows, peram)
    return out[:, :n].reshape(cols, 2, half).transpose(1, 2, 0)


def solution(mesh):
    split = Mesh(
        mesh.devices.reshape(mesh.shape["groups"], NX, NZ, mesh.shape["ea"]),
        ("groups", "gz_0", "gz_1", "ea"),
    )
    in_specs = (
        P("ea", None, None, GROUPS_GZ, None),
        P(None, None, None, None, GROUPS_GZ, None),
        P("groups"),
        P("groups"),
        P("groups", None),
        P("groups", None, None, None, None),
    )
    out_specs = P("groups", "ea", GZ)
    return jax.shard_map(
        shards, mesh=split, in_specs=in_specs, out_specs=out_specs, check_vma=False
    )
```

```python
import functools
import math

import jax
import jax.numpy as jnp
from jax import lax
from jax.experimental import pallas as pl
from jax.experimental.pallas import tpu as pltpu
from jax.sharding import Mesh
from jax.sharding import PartitionSpec as P

LX = 32
LY = 16
NX = 4
NZ = 16
SIDE = 2
GZ = ("gz_0", "gz_1")
GROUPS_GZ = ("groups", "gz_0", "gz_1")
MESH = pl.DeviceIdType.MESH
F32 = jnp.float32
BF16 = jnp.bfloat16


def prepare(half, scale, sizes, ea, along_z, spins, moms, pbuf, mix_ref, left_ref, phase_ref):
    def split(ref, at, value):
        high = value.astype(BF16)
        ref[0, at, :] = high
        ref[1, at, :] = (value - high.astype(F32)).astype(BF16)

    n = pbuf.shape[-1]

    def block(q, part):
        return pbuf[spins[0, q], spins[1, q], part].T

    for slot, q in ((0, 1), (1, 2)):
        re, im = block(q, 0), block(q, 1)
        split(mix_ref.at[slot], slice(0, n), jnp.concatenate([re, -im], 1))
        split(mix_ref.at[slot], slice(n, 2 * n), jnp.concatenate([im, re], 1))
    re = block(0, 0) * scale
    im = block(0, 1) * scale
    first = ea == 0
    pad = jnp.zeros((128 - 2 * half, 2 * n), F32)
    for own in range(2):
        low, high = slice(0, half), slice(half, 2 * half)
        one, two = (low, high) if own == 0 else (high, low)
        r = jnp.where(first, re[one], re[two])
        i = jnp.where(first, im[one], im[two])
        real = jnp.concatenate([r, -i], 1)
        imag = jnp.concatenate([i, r], 1)
        split(left_ref.at[0], slice(own * 128, own * 128 + 128), jnp.concatenate([real, imag, pad], 0))
        split(left_ref.at[1], slice(own * 128, own * 128 + 128), jnp.concatenate([-imag, real, pad], 0))
    lx, ly, depth = sizes
    sites = lax.broadcasted_iota(jnp.int32, (8, lx * ly), 1)
    xcoord = lax.rem(sites, lx)
    ycoord = lax.div(sites, lx)
    two_pi = 2.0 * math.pi
    inplane = (moms[0] * xcoord).astype(F32) / lx + (moms[1] * ycoord).astype(F32) / ly
    along = jnp.full((8, lx * ly), moms[2] * along_z, jnp.int32).astype(F32)
    angle = two_pi * inplane + two_pi * along / depth
    phase_ref[0] = jnp.cos(angle)
    phase_ref[1] = jnp.sin(angle)


def times(lr, li, vr, vi):
    return lr * vr - li * vi, lr * vi + li * vr


def times_conj(lr, li, vr, vi):
    return lr * vr + li * vi, lr * vi - li * vr


def main_kernel(
    scale, weights, spins, moms, v_ref, links, peram, out_ref,
    pbuf, phase, mix, left,
    vall, upper, lower, back, disp, phown, phall, v1, v2, lmat, wbuf0, wbuf1, acc,
    grid_in, mine, grid_out, far_in, mid_out, x_in, near_out, near_in, near_own, ring_out, plus_in, minus_in, short_out, plus_short, minus_short,
    p_sem, halo_s, halo_r, ea_s, ea_r, dd_s, dd_r, fx_s, fx_r, x_s, x_r, near_s, near_r, plus_s, plus_r, minus_s, minus_r,
):
    ncomp, half, plane = v_ref.shape
    cols = out_ref.shape[0]
    packed = far_in.shape[1]
    tiles = cols // 16
    per_row = 2 * half // 16
    x = lax.axis_index("gz_0")
    z = lax.axis_index("gz_1")
    e = lax.axis_index("ea")
    nx = lax.axis_size("gz_0")
    nz = lax.axis_size("gz_1")
    sgn = 1 - 2 * e
    xp = lax.rem(x + sgn + nx, nx)
    xm = lax.rem(x - sgn + nx, nx)
    zh = z // SIDE
    zl = lax.rem(z, SIDE)
    partner = {"ea": 1 - e}
    to_xp = {"gz_0": xp}
    to_xm = {"gz_0": xm}
    gz = x * nz + z
    gup = lax.rem(gz + 1, nx * nz)
    gdn = lax.rem(gz + nx * nz - 1, nx * nz)
    site_up = {"gz_0": gup // nz, "gz_1": lax.rem(gup, nz)}
    site_dn = {"gz_0": gdn // nz, "gz_1": lax.rem(gdn, nz)}

    nh = nz // SIDE
    pair = {"gz_1": zh * SIDE + 1 - zl}
    ring_up = {"gz_1": lax.rem(zh + 1, nh) * SIDE + zl}
    ring_dn = {"gz_1": lax.rem(zh + nh - 1, nh) * SIDE + zl}
    ring = 4

    def remote(src, dst, s, r, to):
        return pltpu.make_async_remote_copy(
            src_ref=src, dst_ref=dst, send_sem=s, recv_sem=r, device_id=to, device_id_type=MESH
        )

    barrier = pltpu.get_barrier_semaphore()
    peers = [partner, to_xp, to_xm, site_up, site_dn]
    peers += [pair, ring_up, ring_dn]
    for to in peers:
        pl.semaphore_signal(barrier, inc=1, device_id=to, device_id_type=MESH)
    pl.semaphore_wait(barrier, len(peers))

    rows = 16
    chunks = half // rows

    def chunk_of(ref, t):
        return ref.at[:, pl.ds(t * rows, rows), :]

    def v_copy(t):
        return remote(
            chunk_of(v_ref, t), chunk_of(upper, t), halo_s.at[0, t], halo_r.at[0, t], site_dn
        )

    def b_copy(t):
        return remote(
            chunk_of(back, t), chunk_of(lower, t), halo_s.at[1, t], halo_r.at[1, t], site_up
        )

    def ph_copy(t):
        return remote(
            chunk_of(phown, t), chunk_of(phall.at[e], t), ea_s.at[1 + t], ea_r.at[1 + t], partner
        )

    for t in range(chunks):
        v_copy(t).start()
    fetch = pltpu.make_async_copy(peram, pbuf, p_sem)
    fetch.start()
    send_ea = remote(v_ref, vall.at[e], ea_s.at[0], ea_r.at[0], partner)
    send_ea.start()

    def field(ref, r0):
        return [ref[c, pl.ds(r0, rows), :].astype(F32) for c in range(ncomp)]

    def link(d, row, col, part):
        return links[((d * 3 + row) * 3 + col) * 2 + part]

    def apply(d, f):
        out = []
        for row in range(3):
            re, im = 0.0, 0.0
            for col in range(3):
                a, b = times(link(d, row, col, 0), link(d, row, col, 1), f[2 * col], f[2 * col + 1])
                re, im = re + a, im + b
            out += [re, im]
        return out

    def adjoint(d, f):
        out = []
        for col in range(3):
            re, im = 0.0, 0.0
            for row in range(3):
                a, b = times_conj(
                    link(d, row, col, 0), link(d, row, col, 1), f[2 * row], f[2 * row + 1]
                )
                re, im = re + a, im + b
            out += [re, im]
        return out

    def back_tile(t):
        r0 = t * rows
        f = field(v_ref, r0)
        for c, val in enumerate(adjoint(2, f)):
            back[c, pl.ds(r0, rows), :] = val.astype(BF16)
        for c in range(ncomp):
            vall[e, c, pl.ds(r0, rows), :] = v_ref[c, pl.ds(r0, rows), :]

    for t in range(chunks):
        back_tile(t)
        b_copy(t).start()
    fetch.wait()
    prepare(half, scale, (LX, LY, nx * nz), e, gz, spins, moms, pbuf, mix, left, phase)

    lane = lax.broadcasted_iota(jnp.int32, (rows, plane), 1)
    xc = lax.rem(lane, LX)

    def shift_x(val, by):
        if by < 0:
            return jnp.where(
                xc == LX - 1, pltpu.roll(val, LX - 1, 1), pltpu.roll(val, plane - 1, 1)
            )
        return jnp.where(xc == 0, pltpu.roll(val, plane - (LX - 1), 1), pltpu.roll(val, 1, 1))

    def shift_y(val, by):
        return pltpu.roll(val, plane - LX if by < 0 else LX, 1)

    def inplane_tile(t, _):
        r0 = pl.multiple_of(t * rows, rows)
        for d, shift in ((0, shift_x), (1, shift_y)):
            f = field(v_ref, r0)
            ahead = apply(d, [shift(c, -1) for c in f])
            behind = [shift(c.astype(BF16).astype(F32), 1) for c in adjoint(d, f)]
            for c in range(ncomp):
                term = weights[d].astype(F32) * (ahead[c] - behind[c])
                if d == 0:
                    disp[c, pl.ds(r0, rows), :] = term
                else:
                    disp[c, pl.ds(r0, rows), :] += term
        return 0

    send_ea.wait()
    for slot, dst in ((0, v1), (1, v2)):
        for k in range(3):
            stack = jnp.concatenate(
                [vall[0, 2 * k], vall[1, 2 * k], vall[0, 2 * k + 1], vall[1, 2 * k + 1]], 0
            )
            res = jnp.dot(mix[slot, 0], stack, preferred_element_type=F32) + jnp.dot(
                mix[slot, 1], stack, preferred_element_type=F32
            )
            for r in range(2):
                part = res[2 * half * r : 2 * half * (r + 1)]
                for lt in range(plane // 128):
                    dst[2 * k + r, lt] = part[:, lt * 128 : lt * 128 + 128]

    def is_minus(step):
        return (step == 3) | (step >= 5)

    def hop_of(step):
        return jnp.where(step < 3, step, jnp.where(step == 3, 0, jnp.where(step == 4, 3, step - 4)))

    def dest_z(q):
        step = q // 2
        hop = hop_of(step)
        to = jnp.where(is_minus(step), zh + 1 - ring + hop + nh, zh + ring - hop)
        return lax.rem(to, nh) * SIDE + jnp.where(lax.rem(q, 2) == 0, 1 - zl, zl)

    turns = 4

    def w_section(dst, step, sec):
        par = sec // 2
        blk = sec - 2 * par
        xd = lax.rem(jnp.where(blk == 0, x + sgn + nx, x + 2 * (1 - e)), nx)
        first = (xd * nz + dest_z(2 * step + par)) * tiles
        row = first // per_row
        skip = first - row * per_row
        for t in range(tiles):
            u = skip + t
            over = jnp.where(u >= per_row, 1, 0) + jnp.where(u >= 2 * per_row, 1, 0)
            b2 = row + over
            c0 = pl.multiple_of((u - over * per_row) * 16, 16)
            row0 = pl.multiple_of(sec * cols + t * 16, 16)
            for lt in range(plane // 128):
                b = [v1[c, lt, pl.ds(b2, 16, stride=0), :] for c in range(ncomp)]
                w = [v2[c, lt, pl.ds(c0, 16), :] for c in range(ncomp)]
                for k, (i, j) in enumerate(((1, 2), (2, 0), (0, 1))):
                    ar, ai, br, bi = b[2 * i], b[2 * i + 1], b[2 * j], b[2 * j + 1]
                    cr, ci, dr, di = w[2 * i], w[2 * i + 1], w[2 * j], w[2 * j + 1]
                    re = ar * dr - ai * di - (br * cr - bi * ci)
                    im = ar * di + ai * dr - (br * ci + bi * cr)
                    for r, val in ((0, re), (1, im)):
                        piece = 2 * (2 * k + r) + lt // 2
                        at = (piece % 3) * 256 + (lt % 2) * 128
                        dst[piece // 3, pl.ds(row0, 16), at : at + 128] = val.astype(BF16)

    def w_only(dst, step):
        lax.fori_loop(0, turns, lambda k, c: (w_section(dst, step, k), 0)[1], 0)

    def dot_turn(src, k):
        acc[...] += jnp.dot(src[k], lmat[k], preferred_element_type=F32)

    def fused(src, dst, step, part):
        if part == 0:
            acc[...] = jnp.zeros_like(acc)

        def turn(k, _):
            dot_turn(src, k)
            w_section(dst, step + 1, k)
            return 0

        lax.fori_loop(part * 2, part * 2 + 2, turn, 0)

    def dot_only(src):
        acc[...] = jnp.zeros_like(acc)
        lax.fori_loop(0, turns, lambda k, c: (dot_turn(src, k), 0)[1], 0)

    def to_partner(q, blk):
        role = 1 if blk == 0 else 2 + e
        return remote(
            grid_out.at[q, blk], grid_in.at[q, role], dd_s.at[q, blk], dd_r.at[q, blk], partner
        )

    fill = lax.broadcasted_iota(jnp.int32, (32, 128), 1) < 2 * half

    def pack(rows_at, lanes):
        for g in range(3):
            extra = acc[rows_at + packed : rows_at + cols, lanes]
            extra = pltpu.roll(extra, 2 * half - 32 * g, 1)
            yield jnp.where(fill, acc[rows_at + 32 * g : rows_at + 32 * g + 32, lanes], extra)
        yield acc[rows_at + 96 : rows_at + packed, lanes]

    def put(ref, pieces):
        at = 0
        for piece in pieces:
            ref[at : at + piece.shape[0], :] = piece.astype(BF16)
            at += piece.shape[0]

    def give(step):
        for par in range(2):
            for blk in range(2):
                q = 2 * step + par
                rows_at = (2 * par + blk) * cols
                put(grid_out.at[q, blk], pack(rows_at, slice(128, 256)))
                to_partner(q, blk).start()
                put(mine.at[q, blk], pack(rows_at, slice(0, 128)))

    def far_copy(q):
        return remote(grid_in.at[q, 2], far_in.at[q], fx_s.at[q], fx_r.at[q], to_xp)

    def far_mine(q):
        return remote(mine.at[q, 1], far_in.at[q], fx_s.at[q], fx_r.at[q], to_xp)

    def direct_copy(q):
        return remote(grid_in.at[q, 1], x_in.at[q, 0], x_s.at[q, 0], x_r.at[q, 0], to_xm)

    def mid_copy(q):
        return remote(mid_out.at[q], x_in.at[q, 1], x_s.at[q, 1], x_r.at[q, 1], to_xp)

    def first_x(q):
        to_partner(q, 0).wait_recv()
        to_partner(q, 1).wait_recv()

        @pl.when(e == 0)
        def _():
            far_mine(q).start()

        @pl.when(e == 1)
        def _():
            far_copy(q).start()

        direct_copy(q).start()

    def second_x(q):
        far_mine(q).wait_recv()
        mid_out[q] = (mine[q, 0].astype(F32) + far_in[q].astype(F32)).astype(BF16)
        mid_copy(q).start()

    def x_sum(q):
        direct_copy(q).wait_recv()
        mid_copy(q).wait_recv()
        total = x_in[q, 0].astype(F32) + x_in[q, 1].astype(F32)
        own = jnp.where(e == 0, grid_in[q, 3].astype(F32), mine[q, 1].astype(F32))
        return total + own

    last = 7

    def near_copy(step):
        return remote(near_out.at[step], near_in.at[step], near_s.at[step], near_r.at[step], pair)

    def near_sum(step):
        near_out[step] = x_sum(2 * step).astype(BF16)
        near_copy(step).start()
        near_own[step] = x_sum(2 * step + 1)

    early = 2
    ring_s, ring_r = (plus_s, minus_s), (plus_r, minus_r)
    ring_to = (ring_up, ring_dn)
    short_in, full_in = (plus_short, minus_short), (plus_in, minus_in)

    def short_copy(side, hop):
        return remote(
            short_out.at[side, hop], short_in[side].at[hop],
            ring_s[side].at[hop], ring_r[side].at[hop], ring_to[side],
        )

    def full_copy(side, hop):
        return remote(
            ring_out.at[side, hop], full_in[side].at[hop],
            ring_s[side].at[hop], ring_r[side].at[hop], ring_to[side],
        )

    def ring_step(side, hop, step):
        near_copy(step).wait_recv()
        ring_out[side, hop] = near_own[step] + near_in[step].astype(F32)

        @pl.when((hop > 0) & (hop <= early))
        def _():
            short_copy(side, hop - 1).wait_recv()
            ring_out[side, hop] += short_in[side][hop - 1].astype(F32)

        @pl.when(hop > early)
        def _():
            full_copy(side, hop - 1).wait_recv()
            ring_out[side, hop] += full_in[side][hop - 1]

        @pl.when(hop < early)
        def _():
            short_out[side, hop] = ring_out[side, hop].astype(BF16)
            short_copy(side, hop).start()

        @pl.when((hop >= early) & (hop < ring - side))
        def _():
            full_copy(side, hop).start()

    w_only(wbuf0, 0)
    lax.fori_loop(0, half // rows, inplane_tile, 0)
    cosine = phase[0, 0:1]
    sine = phase[1, 0:1]

    def zdir_tile(t):
        r0 = t * rows
        ahead = apply(2, field(upper, r0))
        low = field(lower, r0)
        tot = [
            disp[c, pl.ds(r0, rows), :] + weights[2].astype(F32) * (ahead[c] - low[c])
            for c in range(ncomp)
        ]
        for k in range(3):
            re, im = tot[2 * k], tot[2 * k + 1]
            phown[2 * k, pl.ds(r0, rows), :] = (cosine * re + sine * im).astype(BF16)
            phown[2 * k + 1, pl.ds(r0, rows), :] = (cosine * im - sine * re).astype(BF16)
        for c in range(ncomp):
            phall[e, c, pl.ds(r0, rows), :] = phown[c, pl.ds(r0, rows), :]

    for t in range(chunks):
        v_copy(t).wait_recv()
        b_copy(t).wait_recv()
        zdir_tile(t)
        ph_copy(t).start()
    for t in range(chunks):
        ph_copy(t).wait_recv()
    for k in range(3):
        stack = jnp.concatenate(
            [phall[0, 2 * k], phall[1, 2 * k], phall[0, 2 * k + 1], phall[1, 2 * k + 1]], 0
        )
        for r in range(2):
            res = jnp.dot(left[r, 0], stack, preferred_element_type=F32) + jnp.dot(
                left[r, 1], stack, preferred_element_type=F32
            )
            turned = res.T.astype(BF16)
            for hf in range(2):
                piece = 2 * (2 * k + r) + hf
                at = (piece % 3) * 256
                lmat[piece // 3, at : at + 256, :] = turned[hf * 256 : hf * 256 + 256]

    def stage(step, src, dst):
        @pl.when(step < last)
        def _():
            fused(src, dst, step, 0)

        @pl.when((step >= 1) & (step <= last + 1))
        def _():
            first_x(2 * (step - 1))
            first_x(2 * (step - 1) + 1)

        @pl.when((step >= 4) & (step <= last + 4))
        def _():
            near_sum(step - 4)

        @pl.when(step < last)
        def _():
            fused(src, dst, step, 1)

        @pl.when(step == last)
        def _():
            dot_only(src)

        @pl.when(step <= last)
        def _():
            give(step)

        @pl.when((step >= 2) & (step <= last + 2))
        def _():
            second_x(2 * (step - 2))
            second_x(2 * (step - 2) + 1)

    def ring_at(step):
        inside = (step >= 0) & (step <= last)

        @pl.when(inside & jnp.logical_not(is_minus(step)))
        def _():
            ring_step(0, hop_of(step), step)

        @pl.when(inside & is_minus(step))
        def _():
            ring_step(1, hop_of(step), step)

    def body(i, _):
        stage(2 * i, wbuf0, wbuf1)

        ring_at(2 * i - 5)
        stage(2 * i + 1, wbuf1, wbuf0)

        ring_at(2 * i - 4)
        return 0

    lax.fori_loop(0, 7, body, 0)
    full_copy(0, ring - 1).wait_recv()
    total = ring_out[1, ring - 1] + plus_in[ring - 1]
    out_ref[0:packed, :] = total
    spot = lax.broadcasted_iota(jnp.int32, (32, 128), 1)
    extra = jnp.zeros((32, 128), F32)
    for g in range(3):
        piece = pltpu.roll(total[32 * g : 32 * g + 32], (128 - 2 * half + 32 * g) % 128, 1)
        extra = jnp.where((spot >= 32 * g) & (spot < 32 * g + 32), piece, extra)
    out_ref[packed:cols, :] = extra

    def drain(q, _):
        to_partner(q, 0).wait_send()
        to_partner(q, 1).wait_send()
        far_mine(q).wait_send()
        direct_copy(q).wait_send()
        mid_copy(q).wait_send()

        return 0

    lax.fori_loop(0, 2 * (last + 1), drain, 0)
    for t in range(chunks):
        v_copy(t).wait_send()
        b_copy(t).wait_send()
        ph_copy(t).wait_send()
    for step in range(last + 1):
        near_copy(step).wait_send()
    for side in range(2):
        for hop in range(ring - side):
            (short_copy if hop < early else full_copy)(side, hop).wait_send()


def shards(eigvec, links, momentum, weights, spins, peram):
    half = eigvec.shape[0]
    plane = eigvec.shape[4]
    n = 2 * half
    nx, nz, cores = lax.axis_size("gz_0"), lax.axis_size("gz_1"), lax.axis_size("ea")
    depth = nx * nz
    cols = n * n // depth
    scale = 1.0 / math.sqrt(LX * LY * depth)
    fields = eigvec.reshape(half, 6, plane).transpose(1, 0, 2)
    link_rows = links.reshape(54, 1, plane)
    vm = pl.BlockSpec(memory_space=pltpu.VMEM)
    dma = pltpu.SemaphoreType.DMA
    nq = nz
    packed = cols - 32
    out = pl.pallas_call(
        functools.partial(main_kernel, scale),
        out_shape=jax.ShapeDtypeStruct((cols, 128), F32),
        in_specs=[pl.BlockSpec(memory_space=pltpu.SMEM)] * 3 + [vm] * 2 + [pl.BlockSpec(memory_space=pl.ANY)],
        out_specs=vm,
        scratch_shapes=[
            pltpu.VMEM(peram.shape, F32),
            pltpu.VMEM((2, 8, plane), F32),
            pltpu.VMEM((2, 2, 2 * n, 2 * n), BF16),
            pltpu.VMEM((2, 2, 256, 2 * n), BF16),
            pltpu.VMEM((2, 6, half, plane), BF16),
            pltpu.VMEM((6, half, plane), BF16),
            pltpu.VMEM((6, half, plane), BF16),
            pltpu.VMEM((6, half, plane), BF16),
            pltpu.VMEM((6, half, plane), F32),
            pltpu.VMEM((6, half, plane), BF16),
            pltpu.VMEM((2, 6, half, plane), BF16),
            pltpu.VMEM((6, plane // 128, n, 128), F32),
            pltpu.VMEM((6, plane // 128, n, 128), F32),
            pltpu.VMEM((4, 768, 256), BF16),
            pltpu.VMEM((4, 4 * cols, 768), BF16),
            pltpu.VMEM((4, 4 * cols, 768), BF16),
            pltpu.VMEM((4 * cols, 256), F32),
            pltpu.VMEM((nq, 4, packed, 128), BF16),
            pltpu.VMEM((nq, 2, packed, 128), BF16),
            pltpu.VMEM((nq, 2, packed, 128), BF16),
            pltpu.VMEM((nq, packed, 128), BF16),
            pltpu.VMEM((nq, packed, 128), BF16),
            pltpu.VMEM((nq, 2, packed, 128), BF16),
            pltpu.VMEM((8, packed, 128), BF16),
            pltpu.VMEM((8, packed, 128), BF16),
            pltpu.VMEM((8, packed, 128), F32),
            pltpu.VMEM((2, 4, packed, 128), F32),
            pltpu.VMEM((4, packed, 128), F32),
            pltpu.VMEM((4, packed, 128), F32),
            pltpu.VMEM((2, 2, packed, 128), BF16),
            pltpu.VMEM((2, packed, 128), BF16),
            pltpu.VMEM((2, packed, 128), BF16),
            dma, dma((2, 3)), dma((2, 3)), dma((4,)), dma((4,)),
            dma((nq, 2)), dma((nq, 2)), dma((nq,)), dma((nq,)),
            dma((nq, 2)), dma((nq, 2)), dma((8,)), dma((8,)), dma((4,)), dma((4,)), dma((4,)), dma((4,)),
        ],
        compiler_params=pltpu.CompilerParams(
            collective_id=0, has_side_effects=True, vmem_limit_bytes=60 * 1024 * 1024
        ),
    )(weights, spins.T, momentum, fields, link_rows, peram)
    return out[:, :n].reshape(cols, 2, half).transpose(1, 2, 0)


def solution(mesh):
    split = Mesh(
        mesh.devices.reshape(mesh.shape["groups"], NX, NZ, mesh.shape["ea"]),
        ("groups", "gz_0", "gz_1", "ea"),
    )
    in_specs = (
        P("ea", None, None, GROUPS_GZ, None),
        P(None, None, None, None, GROUPS_GZ, None),
        P("groups"),
        P("groups"),
        P("groups", None),
        P("groups", None, None, None, None),
    )
    out_specs = P("groups", "ea", GZ)
    return jax.shard_map(
        shards, mesh=split, in_specs=in_specs, out_specs=out_specs, check_vma=False
    )
```

```python
import functools
import math

import jax
import jax.numpy as jnp
from jax import lax
from jax.experimental import pallas as pl
from jax.experimental.pallas import tpu as pltpu
from jax.sharding import Mesh
from jax.sharding import PartitionSpec as P

LX = 32
LY = 16
NX = 4
NZ = 16
SIDE = 2
GZ = ("gz_0", "gz_1")
GROUPS_GZ = ("groups", "gz_0", "gz_1")
MESH = pl.DeviceIdType.MESH
F32 = jnp.float32
BF16 = jnp.bfloat16


def prepare(half, scale, sizes, ea, along_z, spins, moms, pbuf, mix_ref, left_ref, phase_ref):
    def split(ref, at, value):
        high = value.astype(BF16)
        ref[0, at, :] = high
        ref[1, at, :] = (value - high.astype(F32)).astype(BF16)

    n = pbuf.shape[-1]

    def block(q, part):
        return pbuf[spins[0, q], spins[1, q], part].T

    for slot, q in ((0, 1), (1, 2)):
        re, im = block(q, 0), block(q, 1)
        split(mix_ref.at[slot], slice(0, n), jnp.concatenate([re, -im], 1))
        split(mix_ref.at[slot], slice(n, 2 * n), jnp.concatenate([im, re], 1))
    re = block(0, 0) * scale
    im = block(0, 1) * scale
    first = ea == 0
    pad = jnp.zeros((128 - 2 * half, 2 * n), F32)
    for own in range(2):
        low, high = slice(0, half), slice(half, 2 * half)
        one, two = (low, high) if own == 0 else (high, low)
        r = jnp.where(first, re[one], re[two])
        i = jnp.where(first, im[one], im[two])
        real = jnp.concatenate([r, -i], 1)
        imag = jnp.concatenate([i, r], 1)
        split(left_ref.at[0], slice(own * 128, own * 128 + 128), jnp.concatenate([real, imag, pad], 0))
        split(left_ref.at[1], slice(own * 128, own * 128 + 128), jnp.concatenate([-imag, real, pad], 0))
    lx, ly, depth = sizes
    sites = lax.broadcasted_iota(jnp.int32, (8, lx * ly), 1)
    xcoord = lax.rem(sites, lx)
    ycoord = lax.div(sites, lx)
    two_pi = 2.0 * math.pi
    inplane = (moms[0] * xcoord).astype(F32) / lx + (moms[1] * ycoord).astype(F32) / ly
    along = jnp.full((8, lx * ly), moms[2] * along_z, jnp.int32).astype(F32)
    angle = two_pi * inplane + two_pi * along / depth
    phase_ref[0] = jnp.cos(angle)
    phase_ref[1] = jnp.sin(angle)


def times(lr, li, vr, vi):
    return lr * vr - li * vi, lr * vi + li * vr


def times_conj(lr, li, vr, vi):
    return lr * vr + li * vi, lr * vi - li * vr


def main_kernel(
    scale, weights, spins, moms, v_ref, links, peram, out_ref,
    pbuf, phase, mix, left,
    vall, upper, lower, back, disp, phown, phall, v1, v2, lmat, wbuf0, wbuf1, wbuf2, acc,
    grid_in, mine, grid_out, far_in, mid_out, x_in, near_out, near_in, near_own, ring_out, plus_in, minus_in, short_out, plus_short, minus_short,
    p_sem, halo_s, halo_r, ea_s, ea_r, dd_s, dd_r, fx_s, fx_r, x_s, x_r, near_s, near_r, plus_s, plus_r, minus_s, minus_r,
):
    ncomp, half, plane = v_ref.shape
    cols = out_ref.shape[0]
    packed = far_in.shape[1]
    tiles = cols // 16
    per_row = 2 * half // 16
    x = lax.axis_index("gz_0")
    z = lax.axis_index("gz_1")
    e = lax.axis_index("ea")
    nx = lax.axis_size("gz_0")
    nz = lax.axis_size("gz_1")
    sgn = 1 - 2 * e
    xp = lax.rem(x + sgn + nx, nx)
    xm = lax.rem(x - sgn + nx, nx)
    zh = z // SIDE
    zl = lax.rem(z, SIDE)
    partner = {"ea": 1 - e}
    to_xp = {"gz_0": xp}
    to_xm = {"gz_0": xm}
    gz = x * nz + z
    gup = lax.rem(gz + 1, nx * nz)
    gdn = lax.rem(gz + nx * nz - 1, nx * nz)
    site_up = {"gz_0": gup // nz, "gz_1": lax.rem(gup, nz)}
    site_dn = {"gz_0": gdn // nz, "gz_1": lax.rem(gdn, nz)}

    nh = nz // SIDE
    pair = {"gz_1": zh * SIDE + 1 - zl}
    ring_up = {"gz_1": lax.rem(zh + 1, nh) * SIDE + zl}
    ring_dn = {"gz_1": lax.rem(zh + nh - 1, nh) * SIDE + zl}
    ring = 4

    def remote(src, dst, s, r, to):
        return pltpu.make_async_remote_copy(
            src_ref=src, dst_ref=dst, send_sem=s, recv_sem=r, device_id=to, device_id_type=MESH
        )

    barrier = pltpu.get_barrier_semaphore()
    peers = [partner, to_xp, to_xm, site_up, site_dn]
    peers += [pair, ring_up, ring_dn]
    for to in peers:
        pl.semaphore_signal(barrier, inc=1, device_id=to, device_id_type=MESH)
    pl.semaphore_wait(barrier, len(peers))

    rows = 16
    chunks = half // rows

    def chunk_of(ref, t):
        return ref.at[:, pl.ds(t * rows, rows), :]

    def v_copy(t):
        return remote(
            chunk_of(v_ref, t), chunk_of(upper, t), halo_s.at[0, t], halo_r.at[0, t], site_dn
        )

    def b_copy(t):
        return remote(
            chunk_of(back, t), chunk_of(lower, t), halo_s.at[1, t], halo_r.at[1, t], site_up
        )

    def ph_copy(t):
        return remote(
            chunk_of(phown, t), chunk_of(phall.at[e], t), ea_s.at[1 + t], ea_r.at[1 + t], partner
        )

    for t in range(chunks):
        v_copy(t).start()
    fetch = pltpu.make_async_copy(peram, pbuf, p_sem)
    fetch.start()
    send_ea = remote(v_ref, vall.at[e], ea_s.at[0], ea_r.at[0], partner)
    send_ea.start()

    def field(ref, r0):
        return [ref[c, pl.ds(r0, rows), :].astype(F32) for c in range(ncomp)]

    def link(d, row, col, part):
        return links[((d * 3 + row) * 3 + col) * 2 + part]

    def apply(d, f):
        out = []
        for row in range(3):
            re, im = 0.0, 0.0
            for col in range(3):
                a, b = times(link(d, row, col, 0), link(d, row, col, 1), f[2 * col], f[2 * col + 1])
                re, im = re + a, im + b
            out += [re, im]
        return out

    def adjoint(d, f):
        out = []
        for col in range(3):
            re, im = 0.0, 0.0
            for row in range(3):
                a, b = times_conj(
                    link(d, row, col, 0), link(d, row, col, 1), f[2 * row], f[2 * row + 1]
                )
                re, im = re + a, im + b
            out += [re, im]
        return out

    def back_tile(t):
        r0 = t * rows
        f = field(v_ref, r0)
        for c, val in enumerate(adjoint(2, f)):
            back[c, pl.ds(r0, rows), :] = val.astype(BF16)
        for c in range(ncomp):
            vall[e, c, pl.ds(r0, rows), :] = v_ref[c, pl.ds(r0, rows), :]

    for t in range(chunks):
        back_tile(t)
        b_copy(t).start()
    fetch.wait()
    prepare(half, scale, (LX, LY, nx * nz), e, gz, spins, moms, pbuf, mix, left, phase)

    lane = lax.broadcasted_iota(jnp.int32, (rows, plane), 1)
    xc = lax.rem(lane, LX)

    def shift_x(val, by):
        if by < 0:
            return jnp.where(
                xc == LX - 1, pltpu.roll(val, LX - 1, 1), pltpu.roll(val, plane - 1, 1)
            )
        return jnp.where(xc == 0, pltpu.roll(val, plane - (LX - 1), 1), pltpu.roll(val, 1, 1))

    def shift_y(val, by):
        return pltpu.roll(val, plane - LX if by < 0 else LX, 1)

    def inplane_tile(t, _):
        r0 = pl.multiple_of(t * rows, rows)
        for d, shift in ((0, shift_x), (1, shift_y)):
            f = field(v_ref, r0)
            ahead = apply(d, [shift(c, -1) for c in f])
            behind = [shift(c.astype(BF16).astype(F32), 1) for c in adjoint(d, f)]
            for c in range(ncomp):
                term = weights[d].astype(F32) * (ahead[c] - behind[c])
                if d == 0:
                    disp[c, pl.ds(r0, rows), :] = term
                else:
                    disp[c, pl.ds(r0, rows), :] += term
        return 0

    send_ea.wait()
    for slot, dst in ((0, v1), (1, v2)):
        for k in range(3):
            stack = jnp.concatenate(
                [vall[0, 2 * k], vall[1, 2 * k], vall[0, 2 * k + 1], vall[1, 2 * k + 1]], 0
            )
            res = jnp.dot(mix[slot, 0], stack, preferred_element_type=F32) + jnp.dot(
                mix[slot, 1], stack, preferred_element_type=F32
            )
            for r in range(2):
                part = res[2 * half * r : 2 * half * (r + 1)]
                for lt in range(plane // 128):
                    dst[2 * k + r, lt] = part[:, lt * 128 : lt * 128 + 128]

    def is_minus(step):
        return (step == 3) | (step >= 5)

    def hop_of(step):
        return jnp.where(step < 3, step, jnp.where(step == 3, 0, jnp.where(step == 4, 3, step - 4)))

    def dest_z(q):
        step = q // 2
        hop = hop_of(step)
        to = jnp.where(is_minus(step), zh + 1 - ring + hop + nh, zh + ring - hop)
        return lax.rem(to, nh) * SIDE + jnp.where(lax.rem(q, 2) == 0, 1 - zl, zl)

    turns = 4

    def w_section(dst, step, sec):
        par = sec // 2
        blk = sec - 2 * par
        xd = lax.rem(jnp.where(blk == 0, x + sgn + nx, x + 2 * (1 - e)), nx)
        first = (xd * nz + dest_z(2 * step + par)) * tiles
        row = first // per_row
        skip = first - row * per_row
        for t in range(tiles):
            u = skip + t
            over = jnp.where(u >= per_row, 1, 0) + jnp.where(u >= 2 * per_row, 1, 0)
            b2 = row + over
            c0 = pl.multiple_of((u - over * per_row) * 16, 16)
            row0 = pl.multiple_of(sec * cols + t * 16, 16)
            for lt in range(plane // 128):
                b = [v1[c, lt, pl.ds(b2, 16, stride=0), :] for c in range(ncomp)]
                w = [v2[c, lt, pl.ds(c0, 16), :] for c in range(ncomp)]
                for k, (i, j) in enumerate(((1, 2), (2, 0), (0, 1))):
                    ar, ai, br, bi = b[2 * i], b[2 * i + 1], b[2 * j], b[2 * j + 1]
                    cr, ci, dr, di = w[2 * i], w[2 * i + 1], w[2 * j], w[2 * j + 1]
                    re = ar * dr - ai * di - (br * cr - bi * ci)
                    im = ar * di + ai * dr - (br * ci + bi * cr)
                    for r, val in ((0, re), (1, im)):
                        piece = 2 * (2 * k + r) + lt // 2
                        at = (piece % 3) * 256 + (lt % 2) * 128
                        dst[piece // 3, pl.ds(row0, 16), at : at + 128] = val.astype(BF16)

    def w_only(dst, step):
        lax.fori_loop(0, turns, lambda k, c: (w_section(dst, step, k), 0)[1], 0)

    def dot_turn(src, k):
        acc[...] += jnp.dot(src[k], lmat[k], preferred_element_type=F32)

    def fused(src, dst, step, part):
        if part == 0:
            acc[...] = jnp.zeros_like(acc)

        def turn(k, _):
            dot_turn(src, k)
            w_section(dst, step + 2, k)
            return 0

        lax.fori_loop(part * 2, part * 2 + 2, turn, 0)

    def dot_only(src):
        acc[...] = jnp.zeros_like(acc)
        lax.fori_loop(0, turns, lambda k, c: (dot_turn(src, k), 0)[1], 0)

    def to_partner(q, blk):
        role = 1 if blk == 0 else 2 + e
        return remote(
            grid_out.at[q, blk], grid_in.at[q, role], dd_s.at[q, blk], dd_r.at[q, blk], partner
        )

    fill = lax.broadcasted_iota(jnp.int32, (32, 128), 1) < 2 * half

    def pack(rows_at, lanes):
        for g in range(3):
            extra = acc[rows_at + packed : rows_at + cols, lanes]
            extra = pltpu.roll(extra, 2 * half - 32 * g, 1)
            yield jnp.where(fill, acc[rows_at + 32 * g : rows_at + 32 * g + 32, lanes], extra)
        yield acc[rows_at + 96 : rows_at + packed, lanes]

    def put(ref, pieces):
        at = 0
        for piece in pieces:
            ref[at : at + piece.shape[0], :] = piece.astype(BF16)
            at += piece.shape[0]

    def give(step):
        for par in range(2):
            for blk in range(2):
                q = 2 * step + par
                rows_at = (2 * par + blk) * cols
                put(grid_out.at[q, blk], pack(rows_at, slice(128, 256)))
                to_partner(q, blk).start()
                put(mine.at[q, blk], pack(rows_at, slice(0, 128)))

    def far_copy(q):
        return remote(grid_in.at[q, 2], far_in.at[q], fx_s.at[q], fx_r.at[q], to_xp)

    def far_mine(q):
        return remote(mine.at[q, 1], far_in.at[q], fx_s.at[q], fx_r.at[q], to_xp)

    def direct_copy(q):
        return remote(grid_in.at[q, 1], x_in.at[q, 0], x_s.at[q, 0], x_r.at[q, 0], to_xm)

    def mid_copy(q):
        return remote(mid_out.at[q], x_in.at[q, 1], x_s.at[q, 1], x_r.at[q, 1], to_xp)

    def first_x(q):
        to_partner(q, 0).wait_recv()
        to_partner(q, 1).wait_recv()

        @pl.when(e == 0)
        def _():
            far_mine(q).start()

        @pl.when(e == 1)
        def _():
            far_copy(q).start()

        direct_copy(q).start()

    def second_x(q):
        far_mine(q).wait_recv()
        mid_out[q] = (mine[q, 0].astype(F32) + far_in[q].astype(F32)).astype(BF16)
        mid_copy(q).start()

    def x_sum(q):
        direct_copy(q).wait_recv()
        mid_copy(q).wait_recv()
        total = x_in[q, 0].astype(F32) + x_in[q, 1].astype(F32)
        own = jnp.where(e == 0, grid_in[q, 3].astype(F32), mine[q, 1].astype(F32))
        return total + own

    last = 7

    def near_copy(step):
        return remote(near_out.at[step], near_in.at[step], near_s.at[step], near_r.at[step], pair)

    def near_sum(step):
        near_out[step] = x_sum(2 * step).astype(BF16)
        near_copy(step).start()
        near_own[step] = x_sum(2 * step + 1)

    early = 2
    ring_s, ring_r = (plus_s, minus_s), (plus_r, minus_r)
    ring_to = (ring_up, ring_dn)
    short_in, full_in = (plus_short, minus_short), (plus_in, minus_in)

    def short_copy(side, hop):
        return remote(
            short_out.at[side, hop], short_in[side].at[hop],
            ring_s[side].at[hop], ring_r[side].at[hop], ring_to[side],
        )

    def full_copy(side, hop):
        return remote(
            ring_out.at[side, hop], full_in[side].at[hop],
            ring_s[side].at[hop], ring_r[side].at[hop], ring_to[side],
        )

    def ring_step(side, hop, step):
        near_copy(step).wait_recv()
        ring_out[side, hop] = near_own[step] + near_in[step].astype(F32)

        @pl.when((hop > 0) & (hop <= early))
        def _():
            short_copy(side, hop - 1).wait_recv()
            ring_out[side, hop] += short_in[side][hop - 1].astype(F32)

        @pl.when(hop > early)
        def _():
            full_copy(side, hop - 1).wait_recv()
            ring_out[side, hop] += full_in[side][hop - 1]

        @pl.when(hop < early)
        def _():
            short_out[side, hop] = ring_out[side, hop].astype(BF16)
            short_copy(side, hop).start()

        @pl.when((hop >= early) & (hop < ring - side))
        def _():
            full_copy(side, hop).start()

    w_only(wbuf0, 0)
    lax.fori_loop(0, half // rows, inplane_tile, 0)
    w_only(wbuf1, 1)
    cosine = phase[0, 0:1]
    sine = phase[1, 0:1]

    def zdir_tile(t):
        r0 = t * rows
        ahead = apply(2, field(upper, r0))
        low = field(lower, r0)
        tot = [
            disp[c, pl.ds(r0, rows), :] + weights[2].astype(F32) * (ahead[c] - low[c])
            for c in range(ncomp)
        ]
        for k in range(3):
            re, im = tot[2 * k], tot[2 * k + 1]
            phown[2 * k, pl.ds(r0, rows), :] = (cosine * re + sine * im).astype(BF16)
            phown[2 * k + 1, pl.ds(r0, rows), :] = (cosine * im - sine * re).astype(BF16)
        for c in range(ncomp):
            phall[e, c, pl.ds(r0, rows), :] = phown[c, pl.ds(r0, rows), :]

    for t in range(chunks):
        v_copy(t).wait_recv()
        b_copy(t).wait_recv()
        zdir_tile(t)
        ph_copy(t).start()
    for t in range(chunks):
        ph_copy(t).wait_recv()
    for k in range(3):
        stack = jnp.concatenate(
            [phall[0, 2 * k], phall[1, 2 * k], phall[0, 2 * k + 1], phall[1, 2 * k + 1]], 0
        )
        for r in range(2):
            res = jnp.dot(left[r, 0], stack, preferred_element_type=F32) + jnp.dot(
                left[r, 1], stack, preferred_element_type=F32
            )
            turned = res.T.astype(BF16)
            for hf in range(2):
                piece = 2 * (2 * k + r) + hf
                at = (piece % 3) * 256
                lmat[piece // 3, at : at + 256, :] = turned[hf * 256 : hf * 256 + 256]

    def stage(step, src, dst):
        @pl.when(step < last - 1)
        def _():
            fused(src, dst, step, 0)

        @pl.when((step >= 1) & (step <= last + 1))
        def _():
            first_x(2 * (step - 1))
            first_x(2 * (step - 1) + 1)

        @pl.when((step >= 4) & (step <= last + 4))
        def _():
            near_sum(step - 4)

        @pl.when(step < last - 1)
        def _():
            fused(src, dst, step, 1)

        @pl.when((step >= last - 1) & (step <= last))
        def _():
            dot_only(src)

        @pl.when(step <= last)
        def _():
            give(step)

        @pl.when((step >= 2) & (step <= last + 2))
        def _():
            second_x(2 * (step - 2))
            second_x(2 * (step - 2) + 1)

    def ring_at(step):
        inside = (step >= 0) & (step <= last)

        @pl.when(inside & jnp.logical_not(is_minus(step)))
        def _():
            ring_step(0, hop_of(step), step)

        @pl.when(inside & is_minus(step))
        def _():
            ring_step(1, hop_of(step), step)

    bufs = (wbuf0, wbuf1, wbuf2)

    def body(i, _):
        for u in range(3):
            stage(3 * i + u, bufs[u], bufs[(u + 2) % 3])
            ring_at(3 * i + u - 5)
        return 0

    lax.fori_loop(0, 5, body, 0)
    full_copy(0, ring - 1).wait_recv()
    total = ring_out[1, ring - 1] + plus_in[ring - 1]
    out_ref[0:packed, :] = total
    spot = lax.broadcasted_iota(jnp.int32, (32, 128), 1)
    extra = jnp.zeros((32, 128), F32)
    for g in range(3):
        piece = pltpu.roll(total[32 * g : 32 * g + 32], (128 - 2 * half + 32 * g) % 128, 1)
        extra = jnp.where((spot >= 32 * g) & (spot < 32 * g + 32), piece, extra)
    out_ref[packed:cols, :] = extra

    def drain(q, _):
        to_partner(q, 0).wait_send()
        to_partner(q, 1).wait_send()
        far_mine(q).wait_send()
        direct_copy(q).wait_send()
        mid_copy(q).wait_send()

        return 0

    lax.fori_loop(0, 2 * (last + 1), drain, 0)
    for t in range(chunks):
        v_copy(t).wait_send()
        b_copy(t).wait_send()
        ph_copy(t).wait_send()
    for step in range(last + 1):
        near_copy(step).wait_send()
    for side in range(2):
        for hop in range(ring - side):
            (short_copy if hop < early else full_copy)(side, hop).wait_send()


def shards(eigvec, links, momentum, weights, spins, peram):
    half = eigvec.shape[0]
    plane = eigvec.shape[4]
    n = 2 * half
    nx, nz, cores = lax.axis_size("gz_0"), lax.axis_size("gz_1"), lax.axis_size("ea")
    depth = nx * nz
    cols = n * n // depth
    scale = 1.0 / math.sqrt(LX * LY * depth)
    fields = eigvec.reshape(half, 6, plane).transpose(1, 0, 2)
    link_rows = links.reshape(54, 1, plane)
    vm = pl.BlockSpec(memory_space=pltpu.VMEM)
    dma = pltpu.SemaphoreType.DMA
    nq = nz
    packed = cols - 32
    out = pl.pallas_call(
        functools.partial(main_kernel, scale),
        out_shape=jax.ShapeDtypeStruct((cols, 128), F32),
        in_specs=[pl.BlockSpec(memory_space=pltpu.SMEM)] * 3 + [vm] * 2 + [pl.BlockSpec(memory_space=pl.ANY)],
        out_specs=vm,
        scratch_shapes=[
            pltpu.VMEM(peram.shape, F32),
            pltpu.VMEM((2, 8, plane), F32),
            pltpu.VMEM((2, 2, 2 * n, 2 * n), BF16),
            pltpu.VMEM((2, 2, 256, 2 * n), BF16),
            pltpu.VMEM((2, 6, half, plane), BF16),
            pltpu.VMEM((6, half, plane), BF16),
            pltpu.VMEM((6, half, plane), BF16),
            pltpu.VMEM((6, half, plane), BF16),
            pltpu.VMEM((6, half, plane), F32),
            pltpu.VMEM((6, half, plane), BF16),
            pltpu.VMEM((2, 6, half, plane), BF16),
            pltpu.VMEM((6, plane // 128, n, 128), F32),
            pltpu.VMEM((6, plane // 128, n, 128), F32),
            pltpu.VMEM((4, 768, 256), BF16),
            pltpu.VMEM((4, 4 * cols, 768), BF16),
            pltpu.VMEM((4, 4 * cols, 768), BF16),
            pltpu.VMEM((4, 4 * cols, 768), BF16),
            pltpu.VMEM((4 * cols, 256), F32),
            pltpu.VMEM((nq, 4, packed, 128), BF16),
            pltpu.VMEM((nq, 2, packed, 128), BF16),
            pltpu.VMEM((nq, 2, packed, 128), BF16),
            pltpu.VMEM((nq, packed, 128), BF16),
            pltpu.VMEM((nq, packed, 128), BF16),
            pltpu.VMEM((nq, 2, packed, 128), BF16),
            pltpu.VMEM((8, packed, 128), BF16),
            pltpu.VMEM((8, packed, 128), BF16),
            pltpu.VMEM((8, packed, 128), F32),
            pltpu.VMEM((2, 4, packed, 128), F32),
            pltpu.VMEM((4, packed, 128), F32),
            pltpu.VMEM((4, packed, 128), F32),
            pltpu.VMEM((2, 2, packed, 128), BF16),
            pltpu.VMEM((2, packed, 128), BF16),
            pltpu.VMEM((2, packed, 128), BF16),
            dma, dma((2, 3)), dma((2, 3)), dma((4,)), dma((4,)),
            dma((nq, 2)), dma((nq, 2)), dma((nq,)), dma((nq,)),
            dma((nq, 2)), dma((nq, 2)), dma((8,)), dma((8,)), dma((4,)), dma((4,)), dma((4,)), dma((4,)),
        ],
        compiler_params=pltpu.CompilerParams(
            collective_id=0, has_side_effects=True, vmem_limit_bytes=60 * 1024 * 1024
        ),
    )(weights, spins.T, momentum, fields, link_rows, peram)
    return out[:, :n].reshape(cols, 2, half).transpose(1, 2, 0)


def solution(mesh):
    split = Mesh(
        mesh.devices.reshape(mesh.shape["groups"], NX, NZ, mesh.shape["ea"]),
        ("groups", "gz_0", "gz_1", "ea"),
    )
    in_specs = (
        P("ea", None, None, GROUPS_GZ, None),
        P(None, None, None, None, GROUPS_GZ, None),
        P("groups"),
        P("groups"),
        P("groups", None),
        P("groups", None, None, None, None),
    )
    out_specs = P("groups", "ea", GZ)
    return jax.shard_map(
        shards, mesh=split, in_specs=in_specs, out_specs=out_specs, check_vma=False
    )
```
